32 devices in a mesh: blk: 4 (over y, x), grp: 8 (over z, core).
Axes of the slice: x: 2, y: 2, z: 4, core: 2. Of those that a mesh axis runs over, the one named last changes fastest.
Arguments:
- queries: bfloat16 [32, 32, 128], P('blk', 'grp'), may hold values from -3 to 3
- token_counts: int32 [32], P('blk'), may hold values from 8 to 32
- pages: bfloat16 [32, 1024, 128], P(('blk', 'grp')), may hold values from -6 to 6
- patch_counts: int32 [32], P(('blk', 'grp')), may hold values from 512 to 1024
- labels: int32 [32, 32], P(None, ('blk', 'grp')), may hold values 0 or 1
Outputs:
- query_grad: float32 [32, 32, 128], P('blk', 'grp')
- page_grad: float32 [32, 1024, 128], P(('blk', 'grp'))
- page_loss: float32 [32], P(('blk', 'grp'))
The draws below stay inside these ranges and needn't reach their ends.
All inputs are finite; a program needn't handle non-finite values. No bound on the sum of `labels` on one device may be relied on, other than what follows from the above.
Results may differ from the reference program's by a relative error of at most 0.018.
Values may be sent and summed in bfloat16 or wider, within the bound.
A program may use at most 64 MiB of HBM per device.

```python
import jax
import jax.numpy as jnp
from jax import lax

EMBED_DIM = 128
QUERY_TOKENS = 32
PAGE_PATCHES = 1024
QUERY_COUNT = 32
PAGE_COUNT = 32


def page_values(key):
    base = jax.random.normal(jax.random.fold_in(key, 11), (PAGE_COUNT, PAGE_PATCHES, EMBED_DIM), jnp.float32)
    values = base
    return jnp.clip(values, -6.0, 6.0)


def draw_pages(key, part):
    return page_values(key).astype(jnp.bfloat16)


def draw_queries(key, part):
    base = 0.088 * jax.random.normal(jax.random.fold_in(key, 21), (QUERY_COUNT, QUERY_TOKENS, EMBED_DIM), jnp.float32)
    return jnp.clip(base, -3.0, 3.0).astype(jnp.bfloat16)


def set_ends(result, key, least, top_value):
    dims = result.shape
    place = [jax.random.randint(jax.random.fold_in(key, axis), (), 0, dims[axis]) for axis in range(len(dims))]
    result = result.at[tuple(place)].set(least)
    longest = dims.index(max(dims))
    place[longest] = (place[longest] + 1) % dims[longest]
    return result.at[tuple(place)].set(top_value)


def setup_inputs(seed: int = 0) -> dict:
    key_list = jax.random.split(jax.random.key(seed), 6)
    queries = draw_queries(jax.random.fold_in(key_list[5], 71), 0)
    token_counts = set_ends(jax.random.randint(key_list[1], (QUERY_COUNT,), QUERY_TOKENS // 4, QUERY_TOKENS + 1), jax.random.fold_in(key_list[1], 1), QUERY_TOKENS // 4, QUERY_TOKENS).astype(jnp.int32)
    pages = draw_pages(jax.random.fold_in(key_list[5], 71), 0)
    patch_counts = set_ends(jax.random.randint(key_list[3], (PAGE_COUNT,), PAGE_PATCHES // 2, PAGE_PATCHES + 1), jax.random.fold_in(key_list[3], 1), PAGE_PATCHES // 2, PAGE_PATCHES).astype(jnp.int32)
    labels = set_ends((jax.random.randint(key_list[4], (QUERY_COUNT, PAGE_COUNT), 0, 32) < 1).astype(jnp.int32), jax.random.fold_in(key_list[4], 1), 0, 1)
    return {"queries": queries, "token_counts": token_counts, "pages": pages, "patch_counts": patch_counts, "labels": labels}


align_sharpness = 4.0
logit_scale = 2.0
logit_bias = -5.0


def align(query_rows, counts, page_rows, patch_count, label_column):
    query_number = counts.shape[0]
    token_slots = query_rows.shape[0] // query_number
    scores = jnp.dot(query_rows, page_rows.T, preferred_element_type=jnp.float32)
    patch_mask = jnp.arange(page_rows.shape[0]) < patch_count
    logits = jnp.where(patch_mask[None, :], align_sharpness * scores, -jnp.inf)
    row_max = jnp.max(logits, axis=1, keepdims=True)
    exponent = jnp.exp(logits - row_max)
    weights = exponent / jnp.sum(exponent, axis=1, keepdims=True)
    token_score = jnp.sum(weights * scores, axis=1)
    token_mask = jnp.arange(token_slots)[None, :] < counts[:, None]
    count_float = counts.astype(jnp.float32)
    pair_score = jnp.sum(jnp.where(token_mask, token_score.reshape(query_number, token_slots), jnp.float32(0.0)), axis=1) / count_float
    label_sign = 2.0 * label_column.astype(jnp.float32) - 1.0
    pair_logit = logit_scale * pair_score + logit_bias
    loss_sum = jnp.sum(jax.nn.softplus(-label_sign * pair_logit))
    score_grad = -label_sign * logit_scale * jax.nn.sigmoid(-label_sign * pair_logit)
    token_grad = jnp.where(token_mask, (score_grad / count_float)[:, None], jnp.float32(0.0)).reshape(-1)
    scores_grad = (token_grad[:, None] * weights * (1.0 + align_sharpness * (scores - token_score[:, None]))).astype(jnp.bfloat16)
    query_term = jnp.dot(scores_grad, page_rows, preferred_element_type=jnp.float32)
    page_term = jnp.dot(scores_grad.T, query_rows, preferred_element_type=jnp.float32)
    return query_term, page_term, loss_sum


def reference(queries, token_counts, pages, patch_counts, labels):
    query_rows = queries.reshape(-1, queries.shape[2])

    def scan_step(query_total, entries):
        page_rows, patch_count, label_column = entries
        query_term, page_term, loss_sum = align(query_rows, token_counts, page_rows, patch_count, label_column)
        return query_total + query_term, (page_term, loss_sum)

    initial = jnp.zeros(query_rows.shape, jnp.float32)
    query_total, (page_grads, losses) = lax.scan(scan_step, initial, (pages, patch_counts, labels.T))
    page_loss = losses / jnp.float32(queries.shape[0])
    return query_total.reshape(queries.shape), page_grads, page_loss
```

```python
import functools
import math

import jax
import jax.numpy as jnp
from jax import lax
from jax.experimental import pallas as pl
from jax.experimental.pallas import tpu as pltpu
from jax.sharding import PartitionSpec as P

align_sharpness = 4.0
logit_scale = 2.0
logit_bias = -5.0
masked = -1e30
exp2_scale = align_sharpness * math.log2(math.e)
MESH = pl.DeviceIdType.MESH
patch_tile = 256


def partner(position, step, size):
    if size & (size - 1):
        return lax.rem(position + step, size)
    result = 0
    bit = 1
    while bit < size:
        here = lax.rem(position // bit, 2)
        flip = (step // bit) % 2
        result = result + (1 - here if flip else here) * bit
        bit *= 2
    return result


def source(position, step, size):
    if size & (size - 1):
        return lax.rem(position + size - step, size)
    return partner(position, step, size)


def fold(value):
    return value.reshape(-1, 8, value.shape[1])


def kernel(
    blocks, groups, half_queries, slice_tokens,
    query_in, count_in, page_in, patch_count_in, label_in,
    query_grad_ref, page_grad_ref, loss_ref,
    count_ref, page_ref, page_turned, patch_count_ref, label_ref,
    held, query_rows, count_rows, label_rows, extra_rows, bias,
    shifted_ref, exponent_ref, grads, own_term,
    part_send, part_recv, page_send, page_recv, loss_send, loss_recv,
    column_send, column_recv, row_send, row_recv, count_send, count_recv,
    mate_send, mate_recv, near_send, far_send, part_recv_sem,
    page_send_sem, page_recv_sem, loss_send_sem, loss_recv_sem, load_sem,
):
    blk = lax.axis_index("blk")
    grp = lax.axis_index("grp")
    half = lax.rem(grp, 2)
    mate = grp + 1 - 2 * half
    _, patches, width = page_ref.shape
    piece = half_queries * slice_tokens
    rows = piece * groups
    free = patches // 2
    total_queries = blocks * half_queries * 2
    tiles = [pl.ds(start, patch_tile) for start in range(0, patches, patch_tile)]
    tile_folds = patch_tile // 8

    barrier = pltpu.get_barrier_semaphore()
    for step in range(1, groups):
        pl.semaphore_signal(
            barrier, inc=1, device_id=(blk, partner(grp, step, groups)), device_id_type=MESH
        )
    for step in range(blocks - 1, 0, -1):
        pl.semaphore_signal(
            barrier, inc=1, device_id=(partner(blk, step, blocks), grp), device_id_type=MESH
        )

    loads = [
        pltpu.make_async_copy(src, dst, load_sem.at[index])
        for index, (src, dst) in enumerate((
            (count_in, count_ref), (label_in, label_ref), (patch_count_in, patch_count_ref),
            (page_in, page_ref.at[0]), (query_in.at[half], held.at[blk, grp]),
        ))
    ]
    for load in loads:
        load.start()

    def remote(src, dst, send, recv, device):
        pltpu.make_async_remote_copy(
            src_ref=src, dst_ref=dst, send_sem=send, recv_sem=recv,
            device_id=device, device_id_type=MESH,
        ).start()

    def settle(ref, sem):
        pltpu.make_async_copy(ref, ref, sem).wait()

    lane = lax.broadcasted_iota(jnp.int32, (1, rows), 1)
    query_row = lax.rem(lane // slice_tokens, half_queries)
    token_row = lane // piece * slice_tokens + lax.rem(lane, slice_tokens)

    def spread(read):
        result = jnp.zeros((1, rows), jnp.float32)
        for index in range(half_queries):
            result = jnp.where(query_row == index, read(index).astype(jnp.float32), result)
        return result

    for load in loads[:3]:
        load.wait()
    count_rows[blk] = spread(lambda index: count_ref[half * half_queries + index])
    for index in range(blocks):
        first = index * half_queries * 2
        label_rows[0, index] = spread(
            lambda query: label_ref[0, first + half * half_queries + query]
        )
        extra_rows[index] = spread(
            lambda query: label_ref[0, first + (1 - half) * half_queries + query]
        )
    patch_count = patch_count_ref[0].astype(jnp.float32)
    extra_rows[blocks] = jnp.full((1, rows), patch_count, jnp.float32)

    pl.semaphore_wait(barrier, groups - 1 + blocks - 1)

    for step in range(groups - 1, 0, -1):
        target = partner(grp, step, groups)
        remote(
            query_in.at[lax.rem(target, 2)], held.at[blk, grp], column_send, column_recv.at[grp],
            (blk, target),
        )
    for step in range(blocks - 1, 0, -1):
        other = partner(blk, step, blocks)
        remote(query_in.at[half], held.at[blk, grp], row_send, row_recv.at[blk], (other, grp))
        remote(count_rows.at[blk], count_rows.at[blk], count_send, count_recv.at[blk], (other, grp))
    remote(page_in, page_ref.at[1], mate_send.at[0], mate_recv.at[0], (blk, mate))
    remote(extra_rows, label_rows.at[1], mate_send.at[1], mate_recv.at[1], (blk, mate))

    patch = (free + lax.broadcasted_iota(jnp.int32, (patches - free, rows), 0)).astype(jnp.float32)
    same_query = (
        lax.rem(lax.broadcasted_iota(jnp.int32, (rows, rows), 0) // slice_tokens, half_queries)
        == lax.rem(lax.broadcasted_iota(jnp.int32, (rows, rows), 1) // slice_tokens, half_queries)
    )
    same_query = jnp.where(same_query, 1.0, 0.0).astype(jnp.bfloat16)
    loads[3].wait()
    bias[0] = jnp.where(patch < patch_count, 0.0, masked)
    page_turned[0] = page_ref[0].T
    part_recv[blk, grp] = jnp.zeros((piece, width), part_recv.dtype)
    loads[4].wait()

    for step in range(1, groups):
        origin = source(grp, step, groups)
        settle(held.at[blk, origin], column_recv.at[origin])
        for hop in range(blocks - 1, 0, -1):
            remote(
                held.at[blk, origin], held.at[blk, origin], row_send, row_recv.at[blk],
                (partner(blk, hop, blocks), grp),
            )

    settle(page_ref.at[1], mate_recv.at[0])
    settle(label_rows.at[1], mate_recv.at[1])
    bias[1] = jnp.where(patch < label_rows[1, blocks], 0.0, masked)
    page_turned[1] = page_ref[1].T

    def softmax_parts(page, queries):
        parts = []
        for index, tile in enumerate(tiles):
            scores = lax.dot_general(
                page_ref[page, tile, :], queries, (((1,), (1,)), ((), ())),
                preferred_element_type=jnp.float32,
            )
            start = index * patch_tile
            if start >= free:
                scores = scores + bias[page, pl.ds(start - free, patch_tile), :]
            scores = fold(scores)
            top = jnp.max(scores, axis=0)
            shifted = scores - top
            exponent = jnp.exp2(shifted * exp2_scale)
            place = pl.ds(index * tile_folds, tile_folds)
            shifted_ref[page, place] = shifted
            exponent_ref[page, place] = exponent
            parts.append((top, jnp.sum(exponent, axis=0), jnp.sum(exponent * shifted, axis=0)))
        return parts

    def pair_terms(page, parts, origin):
        row_max = parts[0][0]
        for top, _, _ in parts[1:]:
            row_max = jnp.maximum(row_max, top)
        row_max = jnp.max(row_max, axis=0, keepdims=True)
        total = jnp.zeros((8, rows), jnp.float32)
        moment = jnp.zeros((8, rows), jnp.float32)
        scaled = []
        for top, part_total, part_moment in parts:
            gap = top - row_max
            scale = jnp.exp2(gap * exp2_scale)
            total = total + scale * part_total
            moment = moment + scale * (part_moment + gap * part_total)
            scaled.append((gap, scale))
        total = jnp.sum(total, axis=0, keepdims=True)
        shifted_score = jnp.sum(moment, axis=0, keepdims=True) / total
        token_score = shifted_score + row_max

        count_row = count_rows[origin]
        live = token_row.astype(jnp.float32) < count_row
        remaining = jnp.where(live, token_score, 0.0)
        sublane = lax.broadcasted_iota(jnp.int32, (16, rows), 0)
        pieces = jnp.zeros((16, rows), jnp.float32)
        for index in range(3):
            value = remaining.astype(jnp.bfloat16).astype(jnp.float32)
            pieces = jnp.where(sublane == index, value, pieces)
            remaining = remaining - value
        pair_sum = jnp.sum(
            jnp.dot(
                pieces.astype(jnp.bfloat16), same_query, preferred_element_type=jnp.float32
            ),
            axis=0, keepdims=True,
        )
        pair_score = pair_sum / count_row
        label_sign = 2.0 * label_rows[page, origin] - 1.0
        signed = -label_sign * (logit_scale * pair_score + logit_bias)
        decay = jnp.exp(-jnp.abs(signed))
        softplus = jnp.maximum(signed, 0.0) + jnp.log1p(decay)
        sigmoid = jnp.where(signed >= 0.0, 1.0, decay) / (1.0 + decay)
        loss_row = jnp.where(token_row == 0, softplus, 0.0)
        token_grad = jnp.where(live, -label_sign * logit_scale * sigmoid / count_row, 0.0) / total
        lines = []
        for gap, scale in scaled:
            slope = scale * token_grad
            lines.append((
                slope * (1.0 + align_sharpness * (gap - shifted_score)), slope * align_sharpness
            ))
        return lines, loss_row

    def block_terms(order, origin):
        queries = held[origin].reshape(rows, width)
        columns = pl.ds(order * rows, rows)
        query_rows[columns, :] = queries
        parts = [softmax_parts(page, queries) for page in range(2)]
        query_term = jnp.zeros((width, rows), jnp.float32)
        losses = []
        for page in range(2):
            lines, loss_row = pair_terms(page, parts[page], origin)
            losses.append(loss_row)
            for index, (offset, slope) in enumerate(lines):
                place = pl.ds(index * tile_folds, tile_folds)
                tile_grad = exponent_ref[page, place] * (offset + slope * shifted_ref[page, place])
                grads[page, tiles[index], columns] = (
                    tile_grad.reshape(patch_tile, rows).astype(jnp.bfloat16)
                )
            query_term = query_term + jnp.dot(
                page_turned[page], grads[page, :, columns], preferred_element_type=jnp.float32
            )
        return query_term.T, losses

    own, losses = block_terms(0, blk)
    own_term[...] = own.reshape(groups, piece, width)
    part_send[blk] = own.astype(jnp.bfloat16).reshape(groups, piece, width)
    for step in range(groups - 1, 0, -1):
        target = partner(grp, step, groups)
        remote(
            part_send.at[blk, target], part_recv.at[blk, grp], near_send, part_recv_sem.at[blk],
            (blk, target),
        )

    for step in range(blocks - 1):
        origin = step + jnp.where(step >= blk, 1, 0)
        settle(held.at[origin], row_recv.at[origin])
        settle(count_rows.at[origin], count_recv.at[origin])
        query_term, block_losses = block_terms(step + 1, origin)
        losses = [first + second for first, second in zip(losses, block_losses)]
        part_send[origin] = query_term.astype(jnp.bfloat16).reshape(groups, piece, width)
        for target in range(groups):
            remote(
                part_send.at[origin, target], part_recv.at[blk, grp], far_send,
                part_recv_sem.at[blk], (origin, target),
            )

    loss_send[...] = losses[1]
    remote(loss_send, loss_recv, loss_send_sem, loss_recv_sem, (blk, mate))
    for index, tile in enumerate(tiles):
        page_send[tile, :] = jnp.dot(
            grads[1, tile, :], query_rows[...], preferred_element_type=jnp.float32
        ).astype(jnp.bfloat16)
        remote(
            page_send.at[tile], page_recv.at[tile], page_send_sem, page_recv_sem.at[index],
            (blk, mate),
        )
    for tile in tiles:
        page_grad_ref[tile, :] = jnp.dot(
            grads[0, tile, :], query_rows[...], preferred_element_type=jnp.float32
        )
    settle(loss_recv, loss_recv_sem)
    loss_ref[0] = jnp.sum(losses[0] + loss_recv[...]) / jnp.float32(total_queries)
    for index, tile in enumerate(tiles):
        settle(page_recv.at[tile], page_recv_sem.at[index])
        page_grad_ref[tile, :] = page_grad_ref[tile, :] + page_recv[tile, :].astype(jnp.float32)

    sums = [jnp.zeros((piece, width), jnp.float32) for _ in range(2)]
    settle(part_recv.at[blk, pl.ds(0, groups - 1)], part_recv_sem.at[blk])
    for group in range(groups):
        sums[group % 2] = sums[group % 2] + part_recv[blk, group].astype(jnp.float32)
    for step in range(blocks - 1):
        origin = step + jnp.where(step >= blk, 1, 0)
        settle(part_recv.at[origin], part_recv_sem.at[origin])
        for group in range(groups):
            sums[group % 2] = sums[group % 2] + part_recv[origin, group].astype(jnp.float32)
    for index in range(2):
        query_grad_ref[index] = sums[index]
    query_grad_ref[half] = query_grad_ref[half] + own_term[grp]

    settle(held.at[0, pl.ds(0, groups - 1)], column_send)
    settle(held.at[pl.ds(0, blocks - 1)], row_send)
    settle(count_rows.at[pl.ds(0, blocks - 1)], count_send)
    settle(page_ref.at[1], mate_send.at[0])
    settle(extra_rows, mate_send.at[1])
    settle(part_send.at[0, pl.ds(0, groups - 1)], near_send)
    settle(part_send.at[pl.ds(0, blocks - 1)], far_send)
    settle(page_send, page_send_sem)
    settle(loss_send, loss_send_sem)


def write_out(query_grad_in, page_grad_in, loss_in, query_grad_ref, page_grad_ref, loss_ref, sems):
    copies = [
        pltpu.make_async_copy(page_grad_in, page_grad_ref, sems.at[0]),
        pltpu.make_async_copy(query_grad_in, query_grad_ref, sems.at[1]),
        pltpu.make_async_copy(loss_in, loss_ref, sems.at[2]),
    ]
    for copy in copies:
        copy.start()
    for copy in copies:
        copy.wait()


def local(queries, token_counts, pages, patch_counts, labels):
    blocks = lax.axis_size("blk")
    groups = lax.axis_size("grp")
    block_queries, slice_tokens, width = queries.shape
    patches = pages.shape[1]
    half_queries = block_queries // 2
    piece = half_queries * slice_tokens
    rows = piece * groups
    vmem = pl.BlockSpec(memory_space=pltpu.VMEM)
    smem = pl.BlockSpec(memory_space=pltpu.SMEM)
    anywhere = pl.BlockSpec(memory_space=pl.ANY)
    dma = pltpu.SemaphoreType.DMA
    f32, bf16 = jnp.float32, jnp.bfloat16
    query_grad, page_grad, page_loss = pl.pallas_call(
        functools.partial(kernel, blocks, groups, half_queries, slice_tokens),
        out_shape=(
            pltpu.VMEM((2, piece, width), f32),
            pltpu.VMEM((patches, width), f32),
            pltpu.SMEM((1,), f32),
        ),
        in_specs=[anywhere] * 5,
        out_specs=(vmem, vmem, smem),
        scratch_shapes=[
            pltpu.SMEM(token_counts.shape, jnp.int32),
            pltpu.VMEM((2, patches, width), bf16),
            pltpu.VMEM((2, width, patches), bf16),
            pltpu.SMEM((1,), jnp.int32),
            pltpu.SMEM((1, labels.shape[0]), jnp.int32),
            pltpu.VMEM((blocks, groups, piece, width), bf16),
            pltpu.VMEM((blocks * rows, width), bf16),
            pltpu.VMEM((blocks, 1, rows), f32),
            pltpu.VMEM((2, blocks + 1, 1, rows), f32),
            pltpu.VMEM((blocks + 1, 1, rows), f32),
            pltpu.VMEM((2, patches - patches // 2, rows), f32),
            pltpu.VMEM((2, patches // 8, 8, rows), f32),
            pltpu.VMEM((2, patches // 8, 8, rows), f32),
            pltpu.VMEM((2, patches, blocks * rows), bf16),
            pltpu.VMEM((groups, piece, width), f32),
            pltpu.VMEM((blocks, groups, piece, width), bf16),
            pltpu.VMEM((blocks, groups, piece, width), bf16),
            pltpu.VMEM((patches, width), bf16),
            pltpu.VMEM((patches, width), bf16),
            pltpu.VMEM((1, rows), f32),
            pltpu.VMEM((1, rows), f32),
            dma, dma((groups,)), dma, dma((blocks,)), dma, dma((blocks,)),
            dma((2,)), dma((2,)), dma, dma, dma((blocks,)),
            dma, dma((patches // patch_tile,)), dma, dma, dma((5,)),
        ],
        compiler_params=pltpu.CompilerParams(
            collective_id=0, has_side_effects=True, vmem_limit_bytes=60 * 1024 * 1024
        ),
        name="late_interaction",
    )(queries.reshape(2, piece, width), token_counts, pages[0], patch_counts, labels.T)
    query_grad, page_grad, page_loss = pl.pallas_call(
        write_out,
        out_shape=(
            jax.ShapeDtypeStruct((2, piece, width), f32),
            jax.ShapeDtypeStruct((patches, width), f32),
            jax.ShapeDtypeStruct((1,), f32),
        ),
        in_specs=[anywhere] * 3,
        out_specs=(anywhere,) * 3,
        scratch_shapes=[dma((3,))],
        compiler_params=pltpu.CompilerParams(vmem_limit_bytes=1024 * 1024),
        name="write_out",
    )(query_grad, page_grad, page_loss)
    return query_grad.reshape(queries.shape), page_grad[None], page_loss


def solution(mesh):
    in_specs = (
        P("blk", "grp", None),
        P("blk"),
        P(("blk", "grp"), None, None),
        P(("blk", "grp")),
        P(None, ("blk", "grp")),
    )
    out_specs = (P("blk", "grp", None), P(("blk", "grp"), None, None), P(("blk", "grp")))
    return jax.shard_map(local, mesh=mesh, in_specs=in_specs, out_specs=out_specs, check_vma=False)
```

```python
import functools
import math

import jax
import jax.numpy as jnp
from jax import lax
from jax.experimental import pallas as pl
from jax.experimental.pallas import tpu as pltpu
from jax.sharding import PartitionSpec as P

align_sharpness = 4.0
logit_scale = 2.0
logit_bias = -5.0
masked = -1e30
exp2_scale = align_sharpness * math.log2(math.e)
MESH = pl.DeviceIdType.MESH
patch_tile = 256


def partner(position, step, size):
    if size & (size - 1):
        return lax.rem(position + step, size)
    result = 0
    bit = 1
    while bit < size:
        here = lax.rem(position // bit, 2)
        flip = (step // bit) % 2
        result = result + (1 - here if flip else here) * bit
        bit *= 2
    return result


def source(position, step, size):
    if size & (size - 1):
        return lax.rem(position + size - step, size)
    return partner(position, step, size)


def fold(value):
    return value.reshape(-1, 8, value.shape[1])


def kernel(
    blocks, groups, half_queries, slice_tokens,
    query_in, count_in, page_in, patch_count_in, label_in,
    query_grad_ref, page_grad_ref, loss_ref,
    query_ref, count_ref, page_ref, page_turned, patch_count_ref, label_ref,
    held, query_rows, count_rows, label_rows, extra_rows, bias,
    score_ref, shifted_ref, exponent_ref, grads, own_term,
    part_send, part_recv, page_send, page_recv, loss_send, loss_recv,
    column_send, column_recv, row_send, row_recv, count_send, count_recv,
    relay_send, row_ready, column_ready, mate_send, mate_recv, near_send, far_send, part_recv_sem,
    page_send_sem, page_recv_sem, loss_send_sem, loss_recv_sem, load_sem,
):
    blk = lax.axis_index("blk")
    grp = lax.axis_index("grp")
    half = lax.rem(grp, 2)
    mate = grp + 1 - 2 * half
    patches, width = page_in.shape
    piece = half_queries * slice_tokens
    rows = piece * groups
    free = patches // 2
    total_queries = blocks * half_queries * 2
    tiles = [pl.ds(start, patch_tile) for start in range(0, patches, patch_tile)]
    tile_folds = patch_tile // 8
    slot = jnp.minimum(grp, 0)
    spans = [pl.ds(start, patches // 2) for start in (0, patches // 2)]
    mine, theirs = pl.ds(0, width), pl.ds(width, width)

    chip = grp // 2
    chips = groups // 2
    barrier = pltpu.get_barrier_semaphore()

    def greet(sem, device):
        pl.semaphore_signal(sem, inc=1, device_id=device, device_id_type=MESH)

    for step in range(1, groups):
        target = partner(grp, step, groups)
        pl.when(target // 2 >= chip - 1)(
            functools.partial(greet, barrier, (blk, target))
        )
    for step in range(1, blocks):
        target = partner(blk, step, blocks)
        pl.when(target > blk)(functools.partial(greet, barrier, (target, grp)))

    loads = [
        pltpu.make_async_copy(src, dst, load_sem.at[index])
        for index, (src, dst) in enumerate((
            (count_in, count_ref), (label_in, label_ref), (patch_count_in, patch_count_ref),
            (query_in, query_ref), (page_in, page_ref.at[:, mine]),
        ))
    ]
    for index in (3, 0, 1, 2, 4):
        loads[index].start()

    def remote(src, dst, send, recv, device):
        pltpu.make_async_remote_copy(
            src_ref=src, dst_ref=dst, send_sem=send, recv_sem=recv,
            device_id=device, device_id_type=MESH,
        ).start()

    def settle(ref, sem):
        pltpu.make_async_copy(ref, ref, sem).wait()

    def give_piece(target):
        remote(
            query_ref.at[lax.rem(target, 2)], held.at[blk, grp], column_send, column_recv.at[chip],
            (blk, target),
        )

    pl.semaphore_wait(barrier, 1 + 2 * chip + 2 * jnp.where(chip + 1 < chips, 1, 0) + blk)
    for step in range(1, blocks):
        target = partner(blk, step, blocks)
        pl.when(target < blk)(functools.partial(greet, row_ready, (target, grp)))
    for step in range(1, groups):
        target = partner(grp, step, groups)
        pl.when((target // 2 <= chip - 2) & (target >= 2))(
            functools.partial(greet, column_ready, (blk, target))
        )
    loads[3].wait()
    for step in range(1, groups):
        target = partner(grp, step, groups)
        pl.when(target // 2 <= chip + 1)(functools.partial(give_piece, target))
    held[blk, grp] = query_ref[half]
    remote(page_in, page_ref.at[:, theirs], mate_send.at[0], mate_recv.at[0], (blk, mate))

    @pl.when((chip > 0) & (chip + 2 < chips))
    def _():
        pl.semaphore_wait(column_ready, 2 * (chips - 2 - chip))
        for step in range(1, groups):
            target = partner(grp, step, groups)
            pl.when(target // 2 > chip + 1)(functools.partial(give_piece, target))

    @pl.when(chip == 1)
    def _():
        pair = held.at[blk, pl.ds(0, 2)]
        settle(pair, column_recv.at[0])
        for target in range(chips - 1, 1, -1):
            remote(pair, pair, relay_send, column_recv.at[0], (blk, 2 * target + half))

    @pl.when(blk + 1 < blocks)
    def _():
        pl.semaphore_wait(row_ready, blocks - 1 - blk)

    for step in range(blocks - 1, 0, -1):
        other = partner(blk, step, blocks)
        remote(query_ref.at[half], held.at[blk, grp], row_send, row_recv.at[blk], (other, grp))

    lane = lax.broadcasted_iota(jnp.int32, (1, rows), 1)
    query_row = lax.rem(lane // slice_tokens, half_queries)
    token_row = lane // piece * slice_tokens + lax.rem(lane, slice_tokens)

    def spread(read):
        result = jnp.zeros((1, rows), jnp.float32)
        for index in range(half_queries):
            result = jnp.where(query_row == index, read(index).astype(jnp.float32), result)
        return result

    for load in loads[:3]:
        load.wait()
    count_rows[blk] = spread(lambda index: count_ref[half * half_queries + index])
    for index in range(blocks):
        first = index * half_queries * 2
        label_rows[0, index] = spread(
            lambda query: label_ref[0, first + half * half_queries + query]
        )
        extra_rows[index] = spread(
            lambda query: label_ref[0, first + (1 - half) * half_queries + query]
        )
    patch_count = patch_count_ref[0].astype(jnp.float32)
    extra_rows[blocks] = jnp.full((1, rows), patch_count, jnp.float32)
    for step in range(blocks - 1, 0, -1):
        other = partner(blk, step, blocks)
        remote(count_rows.at[blk], count_rows.at[blk], count_send, count_recv, (other, grp))
    remote(extra_rows, label_rows.at[1], mate_send.at[1], mate_recv.at[1], (blk, mate))

    patch = (free + lax.broadcasted_iota(jnp.int32, (patches - free, rows), 0)).astype(jnp.float32)
    same_query = (
        lax.rem(lax.broadcasted_iota(jnp.int32, (rows, rows), 0) // slice_tokens, half_queries)
        == lax.rem(lax.broadcasted_iota(jnp.int32, (rows, rows), 1) // slice_tokens, half_queries)
    )
    same_query = jnp.where(same_query, 1.0, 0.0).astype(jnp.bfloat16)
    loads[4].wait()
    bias[:, pl.ds(0, rows)] = jnp.where(patch < patch_count, 0.0, masked)
    page_turned[mine, :] = page_ref[:, mine].T
    part_recv[blk, grp] = jnp.zeros((piece, width), part_recv.dtype)

    def forward(start, size):
        for hop in range(blocks - 1, 0, -1):
            remote(
                held.at[blk, pl.ds(start, size)], held.at[blk, pl.ds(start, size)], row_send,
                row_recv.at[blk], (partner(blk, hop, blocks), grp),
            )

    settle(held.at[blk, mate], column_recv.at[chip])
    forward(mate, 1)
    for step in range(1, chips):
        other = source(chip, step, chips)
        with jax.named_scope("w_col%d" % step):
            pl.when((chip != 1) | (other >= 1))(functools.partial(
                settle, held.at[blk, pl.ds(2 * other, 2)], column_recv.at[other]
            ))

        forward(2 * other, 2)

    settle(page_ref.at[:, theirs], mate_recv.at[0])
    settle(label_rows.at[1], mate_recv.at[1])
    bias[:, pl.ds(rows, rows)] = jnp.where(patch < label_rows[1, blocks], 0.0, masked)
    page_turned[theirs, :] = page_ref[:, theirs].T

    def both(value):
        return jnp.concatenate([value, value], axis=1)

    token_rows = both(token_row)

    def score_pass(query_pair):
        top = None
        for span in spans:
            scores = lax.dot_general(
                page_ref[span, :], query_pair, (((1,), (1,)), ((), ())),
                preferred_element_type=jnp.float32,
            )
            for start in range(0, span.size, patch_tile):
                part = scores[start:start + patch_tile]
                first = span.start + start
                if first >= free:
                    part = part + bias[pl.ds(first - free, patch_tile), :]
                part = fold(part)
                score_ref[0, pl.ds(first // 8, tile_folds)] = part
                part_top = jnp.max(part, axis=0)
                top = part_top if top is None else jnp.maximum(top, part_top)
        return top

    def exponent_pass(top):
        total = jnp.zeros((8, 2 * rows), jnp.float32)
        moment = jnp.zeros((8, 2 * rows), jnp.float32)
        span = patches // 8 // 2

        def body(index, carry):
            place = pl.ds(index * span, span)
            shifted = score_ref[0, place] - top
            exponent = jnp.exp2(shifted * exp2_scale)
            shifted_ref[0, place] = shifted
            exponent_ref[0, place] = exponent
            return (
                carry[0] + jnp.sum(exponent, axis=0), carry[1] + jnp.sum(exponent * shifted, axis=0)
            )

        return lax.fori_loop(0, 2, body, (total, moment))

    def pair_terms(top, total, moment, origin):
        row_max = jnp.max(top, axis=0, keepdims=True)
        gap = top - row_max
        scale = jnp.exp2(gap * exp2_scale)
        moment = scale * (moment + gap * total)
        total = jnp.sum(scale * total, axis=0, keepdims=True)
        shifted_score = jnp.sum(moment, axis=0, keepdims=True) / total
        token_score = shifted_score + row_max

        count_row = both(count_rows[origin])
        live = token_rows.astype(jnp.float32) < count_row
        live_score = jnp.where(live, token_score, 0.0)
        sublane = lax.broadcasted_iota(jnp.int32, (16, rows), 0)
        pieces = jnp.zeros((16, rows), jnp.float32)
        for page in range(2):
            remaining = live_score[:, page * rows:(page + 1) * rows]
            for index in range(3):
                value = remaining.astype(jnp.bfloat16).astype(jnp.float32)
                pieces = jnp.where(sublane == 8 * page + index, value, pieces)
                remaining = remaining - value
        piece_sums = jnp.dot(
            pieces.astype(jnp.bfloat16), same_query, preferred_element_type=jnp.float32
        )
        pair_sum = jnp.concatenate(
            [jnp.sum(piece_sums[8 * page:8 * page + 8], axis=0, keepdims=True) for page in range(2)],
            axis=1,
        )
        pair_score = pair_sum / count_row
        labels = jnp.concatenate([label_rows[0, origin], label_rows[1, origin]], axis=1)
        label_sign = 2.0 * labels - 1.0
        signed = -label_sign * (logit_scale * pair_score + logit_bias)
        decay = jnp.exp(-jnp.abs(signed))
        softplus = jnp.maximum(signed, 0.0) + jnp.log1p(decay)
        sigmoid = jnp.where(signed >= 0.0, 1.0, decay) / (1.0 + decay)
        loss_row = jnp.where(token_rows == 0, softplus, 0.0)
        token_grad = jnp.where(live, -label_sign * logit_scale * sigmoid / count_row, 0.0) / total
        slope = scale * token_grad
        offset = slope * (1.0 + align_sharpness * (gap - shifted_score))
        return offset, slope * align_sharpness, loss_row

    def block_terms(order, origin):
        queries = held[origin].reshape(rows, width)
        empty = jnp.zeros((rows, width), jnp.bfloat16)
        query_pair = jnp.concatenate([
            jnp.concatenate([queries, empty], axis=1), jnp.concatenate([empty, queries], axis=1)
        ], axis=0)
        columns = pl.ds(order * 2 * rows, 2 * rows)
        query_rows[columns, :] = query_pair
        top = score_pass(query_pair)
        offset, slope, loss_row = pair_terms(top, *exponent_pass(top), origin)
        for index, tile in enumerate(tiles):
            place = pl.ds(index * tile_folds, tile_folds)
            tile_grad = exponent_ref[slot, place] * (offset + slope * shifted_ref[slot, place])
            grads[tile, columns] = tile_grad.reshape(patch_tile, 2 * rows).astype(jnp.bfloat16)
        query_term = jnp.zeros((width, rows), jnp.float32)
        for span in spans:
            terms = jnp.dot(
                page_turned[:, span], grads[span, columns], preferred_element_type=jnp.float32
            )
            query_term = query_term + terms[:width, :rows] + terms[width:, rows:]
        return query_term.T, loss_row

    own, losses = block_terms(0, blk)
    own_term[...] = own.reshape(groups, piece, width)
    part_send[blk] = own.astype(jnp.bfloat16).reshape(groups, piece, width)
    for step in range(groups - 1, 0, -1):
        target = partner(grp, step, groups)
        remote(
            part_send.at[blk, target], part_recv.at[blk, grp], near_send, part_recv_sem.at[blk],
            (blk, target),
        )

    for step in range(blocks - 1):
        origin = step + jnp.where(step >= blk, 1, 0)
        settle(held.at[origin], row_recv.at[origin])
        if step == 0:
            settle(count_rows.at[pl.ds(0, blocks - 1)], count_recv)
        query_term, block_losses = block_terms(step + 1, origin)
        losses = losses + block_losses
        part_send[origin] = query_term.astype(jnp.bfloat16).reshape(groups, piece, width)
        for target in range(groups):
            remote(
                part_send.at[origin, target], part_recv.at[blk, grp], far_send,
                part_recv_sem.at[blk], (origin, target),
            )

    loss_send[...] = losses[:, rows:]
    remote(loss_send, loss_recv, loss_send_sem, loss_recv_sem, (blk, mate))
    for span in spans:
        page_terms = jnp.dot(grads[span, :], query_rows[...], preferred_element_type=jnp.float32)
        page_send[span, :] = page_terms[:, width:].astype(jnp.bfloat16)
        page_grad_ref[span, :] = page_terms[:, :width]
        remote(
            page_send.at[span], page_recv.at[span], page_send_sem, page_recv_sem,
            (blk, mate),
        )
    settle(loss_recv, loss_recv_sem)
    loss_ref[0] = jnp.sum(losses[:, :rows] + loss_recv[...]) / jnp.float32(total_queries)
    settle(page_recv, page_recv_sem)
    page_grad_ref[...] = page_grad_ref[...] + page_recv[...].astype(jnp.float32)

    @pl.when(chip > 0)
    def _():
        settle(held.at[0, pl.ds(0, groups - 1)], column_send)

    @pl.when(chip == 0)
    def _():
        settle(held.at[0, pl.ds(0, 3)], column_send)

    @pl.when(chip == 1)
    def _():
        settle(held.at[0, pl.ds(0, 2 * (chips - 2))], relay_send)

    settle(held.at[pl.ds(0, blocks - 1)], row_send)
    settle(count_rows.at[pl.ds(0, blocks - 1)], count_send)
    settle(page_ref.at[:, theirs], mate_send.at[0])
    settle(extra_rows, mate_send.at[1])
    settle(part_send.at[0, pl.ds(0, groups - 1)], near_send)
    settle(part_send.at[pl.ds(0, blocks - 1)], far_send)
    settle(page_send, page_send_sem)
    settle(loss_send, loss_send_sem)

    sums = [jnp.zeros((piece, width), jnp.float32) for _ in range(2)]
    settle(part_recv.at[blk, pl.ds(0, groups - 1)], part_recv_sem.at[blk])
    for group in range(groups):
        sums[group % 2] = sums[group % 2] + part_recv[blk, group].astype(jnp.float32)
    for step in range(blocks - 1):
        origin = step + jnp.where(step >= blk, 1, 0)
        settle(part_recv.at[origin], part_recv_sem.at[origin])
        for group in range(groups):
            sums[group % 2] = sums[group % 2] + part_recv[origin, group].astype(jnp.float32)
    for index in range(2):
        query_grad_ref[index] = sums[index]
    query_grad_ref[half] = query_grad_ref[half] + own_term[grp]


def write_out(query_grad_in, page_grad_in, loss_in, query_grad_ref, page_grad_ref, loss_ref, sems):
    copies = [
        pltpu.make_async_copy(page_grad_in, page_grad_ref, sems.at[0]),
        pltpu.make_async_copy(query_grad_in, query_grad_ref, sems.at[1]),
        pltpu.make_async_copy(loss_in, loss_ref, sems.at[2]),
    ]
    for copy in copies:
        copy.start()
    for copy in copies:
        copy.wait()


def local(queries, token_counts, pages, patch_counts, labels):
    blocks = lax.axis_size("blk")
    groups = lax.axis_size("grp")
    block_queries, slice_tokens, width = queries.shape
    patches = pages.shape[1]
    half_queries = block_queries // 2
    piece = half_queries * slice_tokens
    rows = piece * groups
    vmem = pl.BlockSpec(memory_space=pltpu.VMEM)
    smem = pl.BlockSpec(memory_space=pltpu.SMEM)
    anywhere = pl.BlockSpec(memory_space=pl.ANY)
    dma = pltpu.SemaphoreType.DMA
    f32, bf16 = jnp.float32, jnp.bfloat16
    query_grad, page_grad, page_loss = pl.pallas_call(
        functools.partial(kernel, blocks, groups, half_queries, slice_tokens),
        out_shape=(
            pltpu.VMEM((2, piece, width), f32),
            pltpu.VMEM((patches, width), f32),
            pltpu.SMEM((1,), f32),
        ),
        in_specs=[anywhere] * 5,
        out_specs=(vmem, vmem, smem),
        scratch_shapes=[
            pltpu.VMEM((2, piece, width), bf16),
            pltpu.SMEM(token_counts.shape, jnp.int32),
            pltpu.VMEM((patches, 2 * width), bf16),
            pltpu.VMEM((2 * width, patches), bf16),
            pltpu.SMEM((1,), jnp.int32),
            pltpu.SMEM((1, labels.shape[0]), jnp.int32),
            pltpu.VMEM((blocks, groups, piece, width), bf16),
            pltpu.VMEM((blocks * 2 * rows, 2 * width), bf16),
            pltpu.VMEM((blocks, 1, rows), f32),
            pltpu.VMEM((2, blocks + 1, 1, rows), f32),
            pltpu.VMEM((blocks + 1, 1, rows), f32),
            pltpu.VMEM((patches - patches // 2, 2 * rows), f32),
            pltpu.VMEM((1, patches // 8, 8, 2 * rows), f32),
            pltpu.VMEM((1, patches // 8, 8, 2 * rows), f32),
            pltpu.VMEM((1, patches // 8, 8, 2 * rows), f32),
            pltpu.VMEM((patches, blocks * 2 * rows), bf16),
            pltpu.VMEM((groups, piece, width), f32),
            pltpu.VMEM((blocks, groups, piece, width), bf16),
            pltpu.VMEM((blocks, groups, piece, width), bf16),
            pltpu.VMEM((patches, width), bf16),
            pltpu.VMEM((patches, width), bf16),
            pltpu.VMEM((1, rows), f32),
            pltpu.VMEM((1, rows), f32),
            dma, dma((groups // 2,)), dma, dma((blocks,)), dma, dma,
            dma, pltpu.SemaphoreType.REGULAR, pltpu.SemaphoreType.REGULAR,
            dma((2,)), dma((2,)), dma, dma, dma((blocks,)),
            dma, dma, dma, dma, dma((5,)),
        ],
        compiler_params=pltpu.CompilerParams(
            collective_id=0, has_side_effects=True, vmem_limit_bytes=60 * 1024 * 1024
        ),
        name="late_interaction",
    )(queries.reshape(2, piece, width), token_counts, pages[0], patch_counts, labels.T)
    query_grad, page_grad, page_loss = pl.pallas_call(
        write_out,
        out_shape=(
            jax.ShapeDtypeStruct((2, piece, width), f32),
            jax.ShapeDtypeStruct((patches, width), f32),
            jax.ShapeDtypeStruct((1,), f32),
        ),
        in_specs=[anywhere] * 3,
        out_specs=(anywhere,) * 3,
        scratch_shapes=[dma((3,))],
        compiler_params=pltpu.CompilerParams(vmem_limit_bytes=1024 * 1024),
        name="write_out",
    )(query_grad, page_grad, page_loss)
    return query_grad.reshape(queries.shape), page_grad[None], page_loss


def solution(mesh):
    in_specs = (
        P("blk", "grp", None),
        P("blk"),
        P(("blk", "grp"), None, None),
        P(("blk", "grp")),
        P(None, ("blk", "grp")),
    )
    out_specs = (P("blk", "grp", None), P(("blk", "grp"), None, None), P(("blk", "grp")))
    return jax.shard_map(local, mesh=mesh, in_specs=in_specs, out_specs=out_specs, check_vma=False)
```

```python
import functools
import math

import jax
import jax.numpy as jnp
from jax import lax
from jax.experimental import pallas as pl
from jax.experimental.pallas import tpu as pltpu
from jax.sharding import PartitionSpec as P

align_sharpness = 4.0
logit_scale = 2.0
logit_bias = -5.0
masked = -1e30
exp2_scale = align_sharpness * math.log2(math.e)
MESH = pl.DeviceIdType.MESH
patch_tile = 256


def partner(position, step, size):
    if size & (size - 1):
        return lax.rem(position + step, size)
    result = 0
    bit = 1
    while bit < size:
        here = lax.rem(position // bit, 2)
        flip = (step // bit) % 2
        result = result + (1 - here if flip else here) * bit
        bit *= 2
    return result


def source(position, step, size):
    if size & (size - 1):
        return lax.rem(position + size - step, size)
    return partner(position, step, size)


def fold(value):
    return value.reshape(-1, 8, value.shape[1])


def kernel(
    blocks, groups, half_queries, slice_tokens,
    query_in, count_in, page_in, patch_count_in, label_in,
    query_grad_ref, page_grad_ref, loss_ref,
    query_ref, count_ref, page_ref, page_turned, patch_count_ref, label_ref,
    held, query_rows, token_grads, count_rows, label_rows, extra_rows, bias,
    score_ref, shifted_ref, exponent_ref, grads, own_term,
    part_send, part_recv, page_send, page_recv, loss_send, loss_recv,
    column_send, column_recv, row_send, row_recv, count_send, count_recv,
    relay_send, row_ready, column_ready, mate_send, mate_recv, near_send, far_send, part_recv_sem,
    page_send_sem, page_recv_sem, loss_send_sem, loss_recv_sem, load_sem,
):
    blk = lax.axis_index("blk")
    grp = lax.axis_index("grp")
    half = lax.rem(grp, 2)
    mate = grp + 1 - 2 * half
    patches, width = page_in.shape
    piece = half_queries * slice_tokens
    rows = piece * groups
    free = patches // 2
    total_queries = blocks * half_queries * 2
    tiles = [pl.ds(start, patch_tile) for start in range(0, patches, patch_tile)]
    tile_folds = patch_tile // 8
    slot = jnp.minimum(grp, 0)
    spans = [pl.ds(start, patches // 2) for start in (0, patches // 2)]
    mine, theirs = pl.ds(0, width), pl.ds(width, width)

    chip = grp // 2
    chips = groups // 2
    barrier = pltpu.get_barrier_semaphore()

    def greet(sem, device):
        pl.semaphore_signal(sem, inc=1, device_id=device, device_id_type=MESH)

    for step in range(1, groups):
        target = partner(grp, step, groups)
        pl.when(target // 2 >= chip - 1)(
            functools.partial(greet, barrier, (blk, target))
        )
    for step in range(1, blocks):
        target = partner(blk, step, blocks)
        pl.when(target > blk)(functools.partial(greet, barrier, (target, grp)))

    loads = [
        pltpu.make_async_copy(src, dst, load_sem.at[index])
        for index, (src, dst) in enumerate((
            (count_in, count_ref), (label_in, label_ref), (patch_count_in, patch_count_ref),
            (query_in, query_ref), (page_in, page_ref.at[:, mine]),
        ))
    ]
    for index in (3, 0, 1, 2, 4):
        loads[index].start()

    def remote(src, dst, send, recv, device):
        pltpu.make_async_remote_copy(
            src_ref=src, dst_ref=dst, send_sem=send, recv_sem=recv,
            device_id=device, device_id_type=MESH,
        ).start()

    def settle(ref, sem):
        pltpu.make_async_copy(ref, ref, sem).wait()

    def give_piece(target):
        remote(
            query_ref.at[lax.rem(target, 2)], held.at[blk, grp], column_send, column_recv.at[chip],
            (blk, target),
        )

    pl.semaphore_wait(barrier, 1 + 2 * chip + 2 * jnp.where(chip + 1 < chips, 1, 0) + blk)
    for step in range(1, blocks):
        target = partner(blk, step, blocks)
        pl.when(target < blk)(functools.partial(greet, row_ready, (target, grp)))
    for step in range(1, groups):
        target = partner(grp, step, groups)
        pl.when((target // 2 <= chip - 2) & (target >= 2))(
            functools.partial(greet, column_ready, (blk, target))
        )
    loads[3].wait()
    for step in range(1, groups):
        target = partner(grp, step, groups)
        pl.when(target // 2 <= chip + 1)(functools.partial(give_piece, target))
    held[blk, grp] = query_ref[half]
    remote(page_in, page_ref.at[:, theirs], mate_send.at[0], mate_recv.at[0], (blk, mate))

    @pl.when((chip > 0) & (chip + 2 < chips))
    def _():
        pl.semaphore_wait(column_ready, 2 * (chips - 2 - chip))
        for step in range(1, groups):
            target = partner(grp, step, groups)
            pl.when(target // 2 > chip + 1)(functools.partial(give_piece, target))

    @pl.when(chip == 1)
    def _():
        pair = held.at[blk, pl.ds(0, 2)]
        settle(pair, column_recv.at[0])
        for target in range(chips - 1, 1, -1):
            remote(pair, pair, relay_send, column_recv.at[0], (blk, 2 * target + half))

    @pl.when(blk + 1 < blocks)
    def _():
        pl.semaphore_wait(row_ready, blocks - 1 - blk)

    for step in range(blocks - 1, 0, -1):
        other = partner(blk, step, blocks)
        remote(query_ref.at[half], held.at[blk, grp], row_send, row_recv.at[blk], (other, grp))

    lane = lax.broadcasted_iota(jnp.int32, (1, rows), 1)
    query_row = lax.rem(lane // slice_tokens, half_queries)
    token_row = lane // piece * slice_tokens + lax.rem(lane, slice_tokens)

    def spread(read):
        result = jnp.zeros((1, rows), jnp.float32)
        for index in range(half_queries):
            result = jnp.where(query_row == index, read(index).astype(jnp.float32), result)
        return result

    for load in loads[:3]:
        load.wait()
    count_rows[blk] = spread(lambda index: count_ref[half * half_queries + index])
    for index in range(blocks):
        first = index * half_queries * 2
        label_rows[0, index] = spread(
            lambda query: label_ref[0, first + half * half_queries + query]
        )
        extra_rows[index] = spread(
            lambda query: label_ref[0, first + (1 - half) * half_queries + query]
        )
    patch_count = patch_count_ref[0].astype(jnp.float32)
    extra_rows[blocks] = jnp.full((1, rows), patch_count, jnp.float32)
    for step in range(blocks - 1, 0, -1):
        other = partner(blk, step, blocks)
        remote(count_rows.at[blk], count_rows.at[blk], count_send, count_recv, (other, grp))
    remote(extra_rows, label_rows.at[1], mate_send.at[1], mate_recv.at[1], (blk, mate))

    patch = (free + lax.broadcasted_iota(jnp.int32, (patches - free, rows), 0)).astype(jnp.float32)
    same_query = (
        lax.rem(lax.broadcasted_iota(jnp.int32, (rows, rows), 0) // slice_tokens, half_queries)
        == lax.rem(lax.broadcasted_iota(jnp.int32, (rows, rows), 1) // slice_tokens, half_queries)
    )
    same_query = jnp.where(same_query, 1.0, 0.0).astype(jnp.bfloat16)
    loads[4].wait()
    bias[:, pl.ds(0, rows)] = jnp.where(patch < patch_count, 0.0, masked)
    page_turned[mine, :] = page_ref[:, mine].T
    part_recv[blk, grp] = jnp.zeros((piece, width), part_recv.dtype)
    query_rows[...] = jnp.zeros_like(query_rows)

    def forward(start, size):
        for hop in range(blocks - 1, 0, -1):
            remote(
                held.at[blk, pl.ds(start, size)], held.at[blk, pl.ds(start, size)], row_send,
                row_recv.at[blk], (partner(blk, hop, blocks), grp),
            )

    settle(held.at[blk, mate], column_recv.at[chip])
    forward(mate, 1)
    for step in range(1, chips):
        other = source(chip, step, chips)
        with jax.named_scope("w_col%d" % step):
            pl.when((chip != 1) | (other >= 1))(functools.partial(
                settle, held.at[blk, pl.ds(2 * other, 2)], column_recv.at[other]
            ))

        forward(2 * other, 2)

    settle(page_ref.at[:, theirs], mate_recv.at[0])
    settle(label_rows.at[1], mate_recv.at[1])
    bias[:, pl.ds(rows, rows)] = jnp.where(patch < label_rows[1, blocks], 0.0, masked)
    page_turned[theirs, :] = page_ref[:, theirs].T

    def both(value):
        return jnp.concatenate([value, value], axis=1)

    token_rows = both(token_row)

    def score_pass(query_pair):
        top = None
        for span in spans:
            scores = lax.dot_general(
                page_ref[span, :], query_pair, (((1,), (1,)), ((), ())),
                preferred_element_type=jnp.float32,
            )
            for start in range(0, span.size, patch_tile):
                part = scores[start:start + patch_tile]
                first = span.start + start
                if first >= free:
                    part = part + bias[pl.ds(first - free, patch_tile), :]
                part = fold(part)
                score_ref[0, pl.ds(first // 8, tile_folds)] = part
                part_top = jnp.max(part, axis=0)
                top = part_top if top is None else jnp.maximum(top, part_top)
        return top

    def exponent_pass(top):
        total = jnp.zeros((8, 2 * rows), jnp.float32)
        moment = jnp.zeros((8, 2 * rows), jnp.float32)
        span = patches // 8 // 2

        def body(index, carry):
            place = pl.ds(index * span, span)
            shifted = score_ref[0, place] - top
            exponent = jnp.exp2(shifted * exp2_scale)
            shifted_ref[0, place] = shifted
            exponent_ref[0, place] = exponent
            return (
                carry[0] + jnp.sum(exponent, axis=0), carry[1] + jnp.sum(exponent * shifted, axis=0)
            )

        return lax.fori_loop(0, 2, body, (total, moment))

    def pair_terms(top, total, moment, origin):
        row_max = jnp.max(top, axis=0, keepdims=True)
        gap = top - row_max
        scale = jnp.exp2(gap * exp2_scale)
        moment = scale * (moment + gap * total)
        total = jnp.sum(scale * total, axis=0, keepdims=True)
        shifted_score = jnp.sum(moment, axis=0, keepdims=True) / total
        token_score = shifted_score + row_max

        count_row = both(count_rows[origin])
        live = token_rows.astype(jnp.float32) < count_row
        live_score = jnp.where(live, token_score, 0.0)
        sublane = lax.broadcasted_iota(jnp.int32, (16, rows), 0)
        pieces = jnp.zeros((16, rows), jnp.float32)
        for page in range(2):
            remaining = live_score[:, page * rows:(page + 1) * rows]
            for index in range(3):
                value = remaining.astype(jnp.bfloat16).astype(jnp.float32)
                pieces = jnp.where(sublane == 8 * page + index, value, pieces)
                remaining = remaining - value
        piece_sums = jnp.dot(
            pieces.astype(jnp.bfloat16), same_query, preferred_element_type=jnp.float32
        )
        pair_sum = jnp.concatenate(
            [jnp.sum(piece_sums[8 * page:8 * page + 8], axis=0, keepdims=True) for page in range(2)],
            axis=1,
        )
        pair_score = pair_sum / count_row
        labels = jnp.concatenate([label_rows[0, origin], label_rows[1, origin]], axis=1)
        label_sign = 2.0 * labels - 1.0
        signed = -label_sign * (logit_scale * pair_score + logit_bias)
        decay = jnp.exp(-jnp.abs(signed))
        softplus = jnp.maximum(signed, 0.0) + jnp.log1p(decay)
        sigmoid = jnp.where(signed >= 0.0, 1.0, decay) / (1.0 + decay)
        loss_row = jnp.where(token_rows == 0, softplus, 0.0)
        token_grad = jnp.where(live, -label_sign * logit_scale * sigmoid / count_row, 0.0)
        slope = scale / total
        offset = slope * (1.0 + align_sharpness * (gap - shifted_score))
        return offset, slope * align_sharpness, token_grad, loss_row

    def block_terms(order, origin):
        queries = held[origin].reshape(rows, width)
        empty = jnp.zeros((rows, width), jnp.bfloat16)
        query_pair = jnp.concatenate([
            jnp.concatenate([queries, empty], axis=1), jnp.concatenate([empty, queries], axis=1)
        ], axis=0)
        columns = pl.ds(order * 2 * rows, 2 * rows)
        top = score_pass(query_pair)
        offset, slope, token_grad, loss_row = pair_terms(top, *exponent_pass(top), origin)
        token_grads[order] = token_grad
        for index, tile in enumerate(tiles):
            place = pl.ds(index * tile_folds, tile_folds)
            tile_grad = exponent_ref[slot, place] * (offset + slope * shifted_ref[slot, place])
            grads[tile, columns] = tile_grad.reshape(patch_tile, 2 * rows).astype(jnp.bfloat16)
        query_term = jnp.zeros((width, rows), jnp.float32)
        for span in spans:
            terms = jnp.dot(
                page_turned[:, span], grads[span, columns], preferred_element_type=jnp.float32
            )
            query_term = query_term + (
                terms[:width, :rows] * token_grad[:, :rows] + terms[width:, rows:] * token_grad[:, rows:]
            )
        return query_term.T, loss_row

    own, losses = block_terms(0, blk)
    own_term[...] = own.reshape(groups, piece, width)
    part_send[blk] = own.astype(jnp.bfloat16).reshape(groups, piece, width)
    for step in range(groups - 1, 0, -1):
        target = partner(grp, step, groups)
        remote(
            part_send.at[blk, target], part_recv.at[blk, grp], near_send, part_recv_sem.at[blk],
            (blk, target),
        )

    for step in range(blocks - 1):
        origin = step + jnp.where(step >= blk, 1, 0)
        settle(held.at[origin], row_recv.at[origin])
        if step == 0:
            settle(count_rows.at[pl.ds(0, blocks - 1)], count_recv)
        query_term, block_losses = block_terms(step + 1, origin)
        losses = losses + block_losses
        part_send[origin] = query_term.astype(jnp.bfloat16).reshape(groups, piece, width)
        for target in range(groups):
            remote(
                part_send.at[origin, target], part_recv.at[blk, grp], far_send,
                part_recv_sem.at[blk], (origin, target),
            )

    loss_send[...] = losses[:, rows:]
    remote(loss_send, loss_recv, loss_send_sem, loss_recv_sem, (blk, mate))
    same_row = (
        lax.broadcasted_iota(jnp.int32, (rows, rows), 0)
        == lax.broadcasted_iota(jnp.int32, (rows, rows), 1)
    )
    for order in range(blocks):
        origin = blk if order == 0 else order - 1 + jnp.where(order - 1 >= blk, 1, 0)
        queries = held[origin].reshape(rows, width)
        for page in range(2):
            spread_grad = jnp.where(same_row, token_grads[order, :, page * rows:(page + 1) * rows], 0.0)
            high = spread_grad.astype(jnp.bfloat16)
            low = (spread_grad - high.astype(jnp.float32)).astype(jnp.bfloat16)
            query_rows[
                pl.ds((order * 2 + page) * rows, rows), pl.ds(page * width, width)
            ] = jnp.dot(
                jnp.concatenate([high, low], axis=1), jnp.concatenate([queries, queries], axis=0),
                preferred_element_type=jnp.float32,
            ).astype(jnp.bfloat16)
    for span in spans:
        page_terms = jnp.dot(grads[span, :], query_rows[...], preferred_element_type=jnp.float32)
        page_send[span, :] = page_terms[:, width:].astype(jnp.bfloat16)
        page_grad_ref[span, :] = page_terms[:, :width]
        remote(
            page_send.at[span], page_recv.at[span], page_send_sem, page_recv_sem,
            (blk, mate),
        )
    settle(loss_recv, loss_recv_sem)
    loss_ref[0] = jnp.sum(losses[:, :rows] + loss_recv[...]) / jnp.float32(total_queries)
    settle(page_recv, page_recv_sem)
    page_grad_ref[...] = page_grad_ref[...] + page_recv[...].astype(jnp.float32)

    @pl.when(chip > 0)
    def _():
        settle(held.at[0, pl.ds(0, groups - 1)], column_send)

    @pl.when(chip == 0)
    def _():
        settle(held.at[0, pl.ds(0, 3)], column_send)

    @pl.when(chip == 1)
    def _():
        settle(held.at[0, pl.ds(0, 2 * (chips - 2))], relay_send)

    settle(held.at[pl.ds(0, blocks - 1)], row_send)
    settle(count_rows.at[pl.ds(0, blocks - 1)], count_send)
    settle(page_ref.at[:, theirs], mate_send.at[0])
    settle(extra_rows, mate_send.at[1])
    settle(part_send.at[0, pl.ds(0, groups - 1)], near_send)
    settle(part_send.at[pl.ds(0, blocks - 1)], far_send)
    settle(page_send, page_send_sem)
    settle(loss_send, loss_send_sem)

    sums = [jnp.zeros((piece, width), jnp.float32) for _ in range(2)]
    settle(part_recv.at[blk, pl.ds(0, groups - 1)], part_recv_sem.at[blk])
    for group in range(groups):
        sums[group % 2] = sums[group % 2] + part_recv[blk, group].astype(jnp.float32)
    for step in range(blocks - 1):
        origin = step + jnp.where(step >= blk, 1, 0)
        settle(part_recv.at[origin], part_recv_sem.at[origin])
        for group in range(groups):
            sums[group % 2] = sums[group % 2] + part_recv[origin, group].astype(jnp.float32)
    for index in range(2):
        query_grad_ref[index] = sums[index]
    query_grad_ref[half] = query_grad_ref[half] + own_term[grp]


def write_out(query_grad_in, page_grad_in, loss_in, query_grad_ref, page_grad_ref, loss_ref, sems):
    copies = [
        pltpu.make_async_copy(page_grad_in, page_grad_ref, sems.at[0]),
        pltpu.make_async_copy(query_grad_in, query_grad_ref, sems.at[1]),
        pltpu.make_async_copy(loss_in, loss_ref, sems.at[2]),
    ]
    for copy in copies:
        copy.start()
    for copy in copies:
        copy.wait()


def local(queries, token_counts, pages, patch_counts, labels):
    blocks = lax.axis_size("blk")
    groups = lax.axis_size("grp")
    block_queries, slice_tokens, width = queries.shape
    patches = pages.shape[1]
    half_queries = block_queries // 2
    piece = half_queries * slice_tokens
    rows = piece * groups
    vmem = pl.BlockSpec(memory_space=pltpu.VMEM)
    smem = pl.BlockSpec(memory_space=pltpu.SMEM)
    anywhere = pl.BlockSpec(memory_space=pl.ANY)
    dma = pltpu.SemaphoreType.DMA
    f32, bf16 = jnp.float32, jnp.bfloat16
    query_grad, page_grad, page_loss = pl.pallas_call(
        functools.partial(kernel, blocks, groups, half_queries, slice_tokens),
        out_shape=(
            pltpu.VMEM((2, piece, width), f32),
            pltpu.VMEM((patches, width), f32),
            pltpu.SMEM((1,), f32),
        ),
        in_specs=[anywhere] * 5,
        out_specs=(vmem, vmem, smem),
        scratch_shapes=[
            pltpu.VMEM((2, piece, width), bf16),
            pltpu.SMEM(token_counts.shape, jnp.int32),
            pltpu.VMEM((patches, 2 * width), bf16),
            pltpu.VMEM((2 * width, patches), bf16),
            pltpu.SMEM((1,), jnp.int32),
            pltpu.SMEM((1, labels.shape[0]), jnp.int32),
            pltpu.VMEM((blocks, groups, piece, width), bf16),
            pltpu.VMEM((blocks * 2 * rows, 2 * width), bf16),
            pltpu.VMEM((blocks, 1, 2 * rows), f32),
            pltpu.VMEM((blocks, 1, rows), f32),
            pltpu.VMEM((2, blocks + 1, 1, rows), f32),
            pltpu.VMEM((blocks + 1, 1, rows), f32),
            pltpu.VMEM((patches - patches // 2, 2 * rows), f32),
            pltpu.VMEM((1, patches // 8, 8, 2 * rows), f32),
            pltpu.VMEM((1, patches // 8, 8, 2 * rows), f32),
            pltpu.VMEM((1, patches // 8, 8, 2 * rows), f32),
            pltpu.VMEM((patches, blocks * 2 * rows), bf16),
            pltpu.VMEM((groups, piece, width), f32),
            pltpu.VMEM((blocks, groups, piece, width), bf16),
            pltpu.VMEM((blocks, groups, piece, width), bf16),
            pltpu.VMEM((patches, width), bf16),
            pltpu.VMEM((patches, width), bf16),
            pltpu.VMEM((1, rows), f32),
            pltpu.VMEM((1, rows), f32),
            dma, dma((groups // 2,)), dma, dma((blocks,)), dma, dma,
            dma, pltpu.SemaphoreType.REGULAR, pltpu.SemaphoreType.REGULAR,
            dma((2,)), dma((2,)), dma, dma, dma((blocks,)),
            dma, dma, dma, dma, dma((5,)),
        ],
        compiler_params=pltpu.CompilerParams(
            collective_id=0, has_side_effects=True, vmem_limit_bytes=60 * 1024 * 1024
        ),
        name="late_interaction",
    )(queries.reshape(2, piece, width), token_counts, pages[0], patch_counts, labels.T)
    query_grad, page_grad, page_loss = pl.pallas_call(
        write_out,
        out_shape=(
            jax.ShapeDtypeStruct((2, piece, width), f32),
            jax.ShapeDtypeStruct((patches, width), f32),
            jax.ShapeDtypeStruct((1,), f32),
        ),
        in_specs=[anywhere] * 3,
        out_specs=(anywhere,) * 3,
        scratch_shapes=[dma((3,))],
        compiler_params=pltpu.CompilerParams(vmem_limit_bytes=1024 * 1024),
        name="write_out",
    )(query_grad, page_grad, page_loss)
    return query_grad.reshape(queries.shape), page_grad[None], page_loss


def solution(mesh):
    in_specs = (
        P("blk", "grp", None),
        P("blk"),
        P(("blk", "grp"), None, None),
        P(("blk", "grp")),
        P(None, ("blk", "grp")),
    )
    out_specs = (P("blk", "grp", None), P(("blk", "grp"), None, None), P(("blk", "grp")))
    return jax.shard_map(local, mesh=mesh, in_specs=in_specs, out_specs=out_specs, check_vma=False)
```

```python
import functools
import math

import jax
import jax.numpy as jnp
from jax import lax
from jax.experimental import pallas as pl
from jax.experimental.pallas import tpu as pltpu
from jax.sharding import PartitionSpec as P

align_sharpness = 4.0
logit_scale = 2.0
logit_bias = -5.0
masked = -1e30
exp2_scale = align_sharpness * math.log2(math.e)
MESH = pl.DeviceIdType.MESH
patch_tile = 256


def partner(position, step, size):
    if size & (size - 1):
        return lax.rem(position + step, size)
    result = 0
    bit = 1
    while bit < size:
        here = lax.rem(position // bit, 2)
        flip = (step // bit) % 2
        result = result + (1 - here if flip else here) * bit
        bit *= 2
    return result


def source(position, step, size):
    if size & (size - 1):
        return lax.rem(position + size - step, size)
    return partner(position, step, size)


def fold(value):
    return value.reshape(-1, 8, value.shape[1])


def kernel(
    blocks, groups, half_queries, slice_tokens,
    query_in, count_in, page_in, patch_count_in, label_in,
    query_grad_ref, page_grad_ref, loss_ref,
    query_ref, count_ref, page_ref, page_turned, patch_count_ref, label_ref,
    held, query_rows, token_grads, count_rows, label_rows, extra_rows, bias,
    score_ref, shifted_ref, exponent_ref, grads, own_term,
    part_send, part_recv, page_send, page_recv, loss_send, loss_recv,
    column_send, column_recv, row_send, row_recv, count_send, count_recv,
    relay_send, row_ready, column_ready, mate_send, mate_recv, near_send, far_send, part_recv_sem,
    page_send_sem, page_recv_sem, loss_send_sem, loss_recv_sem, load_sem,
):
    blk = lax.axis_index("blk")
    grp = lax.axis_index("grp")
    half = lax.rem(grp, 2)
    mate = grp + 1 - 2 * half
    patches, width = page_in.shape
    piece = half_queries * slice_tokens
    rows = piece * groups
    free = patches // 2
    total_queries = blocks * half_queries * 2
    tiles = [pl.ds(start, patch_tile) for start in range(0, patches, patch_tile)]
    tile_folds = patch_tile // 8
    slot = jnp.minimum(grp, 0)
    spans = [pl.ds(start, patches // 2) for start in (0, patches // 2)]
    mine, theirs = pl.ds(0, width), pl.ds(width, width)

    chip = grp // 2
    chips = groups // 2
    barrier = pltpu.get_barrier_semaphore()

    def greet(sem, device):
        pl.semaphore_signal(sem, inc=1, device_id=device, device_id_type=MESH)

    for step in range(1, groups):
        target = partner(grp, step, groups)
        pl.when(target // 2 >= chip - 1)(
            functools.partial(greet, barrier, (blk, target))
        )
    for step in range(1, blocks):
        target = partner(blk, step, blocks)
        pl.when(target > blk)(functools.partial(greet, barrier, (target, grp)))

    loads = [
        pltpu.make_async_copy(src, dst, load_sem.at[index])
        for index, (src, dst) in enumerate((
            (count_in, count_ref), (label_in, label_ref), (patch_count_in, patch_count_ref),
            (query_in, query_ref), (page_in, page_ref.at[:, mine]),
        ))
    ]
    for index in (3, 0, 1, 2, 4):
        loads[index].start()

    def remote(src, dst, send, recv, device):
        pltpu.make_async_remote_copy(
            src_ref=src, dst_ref=dst, send_sem=send, recv_sem=recv,
            device_id=device, device_id_type=MESH,
        ).start()

    def settle(ref, sem):
        pltpu.make_async_copy(ref, ref, sem).wait()

    def give_piece(target):
        remote(
            query_ref.at[lax.rem(target, 2)], held.at[blk, grp], column_send, column_recv.at[chip],
            (blk, target),
        )

    pl.semaphore_wait(barrier, 1 + 2 * chip + 2 * jnp.where(chip + 1 < chips, 1, 0) + blk)
    for step in range(1, blocks):
        target = partner(blk, step, blocks)
        pl.when(target < blk)(functools.partial(greet, row_ready, (target, grp)))
    for step in range(1, groups):
        target = partner(grp, step, groups)
        pl.when((target // 2 <= chip - 2) & (target >= 2))(
            functools.partial(greet, column_ready, (blk, target))
        )
    loads[3].wait()
    for step in range(1, groups):
        target = partner(grp, step, groups)
        pl.when(target // 2 <= chip + 1)(functools.partial(give_piece, target))
    held[blk, grp] = query_ref[half]
    remote(page_in, page_ref.at[:, theirs], mate_send.at[0], mate_recv.at[0], (blk, mate))

    @pl.when((chip > 0) & (chip + 2 < chips))
    def _():
        pl.semaphore_wait(column_ready, 2 * (chips - 2 - chip))
        for step in range(1, groups):
            target = partner(grp, step, groups)
            pl.when(target // 2 > chip + 1)(functools.partial(give_piece, target))

    @pl.when(chip == 1)
    def _():
        pair = held.at[blk, pl.ds(0, 2)]
        settle(pair, column_recv.at[0])
        for target in range(chips - 1, 1, -1):
            remote(pair, pair, relay_send, column_recv.at[0], (blk, 2 * target + half))

    @pl.when(blk + 1 < blocks)
    def _():
        pl.semaphore_wait(row_ready, blocks - 1 - blk)

    for step in range(blocks - 1, 0, -1):
        other = partner(blk, step, blocks)
        remote(query_ref.at[half], held.at[blk, grp], row_send, row_recv.at[blk], (other, grp))

    lane = lax.broadcasted_iota(jnp.int32, (1, rows), 1)
    query_row = lax.rem(lane // slice_tokens, half_queries)
    token_row = lane // piece * slice_tokens + lax.rem(lane, slice_tokens)

    def spread(read):
        result = jnp.zeros((1, rows), jnp.float32)
        for index in range(half_queries):
            result = jnp.where(query_row == index, read(index).astype(jnp.float32), result)
        return result

    for load in loads[:3]:
        load.wait()
    count_rows[blk] = spread(lambda index: count_ref[half * half_queries + index])
    for index in range(blocks):
        first = index * half_queries * 2
        label_rows[0, index] = spread(
            lambda query: label_ref[0, first + half * half_queries + query]
        )
        extra_rows[index] = spread(
            lambda query: label_ref[0, first + (1 - half) * half_queries + query]
        )
    patch_count = patch_count_ref[0].astype(jnp.float32)
    extra_rows[blocks] = jnp.full((1, rows), patch_count, jnp.float32)
    for step in range(blocks - 1, 0, -1):
        other = partner(blk, step, blocks)
        remote(count_rows.at[blk], count_rows.at[blk], count_send, count_recv, (other, grp))
    remote(extra_rows, label_rows.at[1], mate_send.at[1], mate_recv.at[1], (blk, mate))

    patch = (free + lax.broadcasted_iota(jnp.int32, (patches - free, rows), 0)).astype(jnp.float32)
    same_query = (
        lax.rem(lax.broadcasted_iota(jnp.int32, (rows, rows), 0) // slice_tokens, half_queries)
        == lax.rem(lax.broadcasted_iota(jnp.int32, (rows, rows), 1) // slice_tokens, half_queries)
    )
    same_query = jnp.where(same_query, 1.0, 0.0).astype(jnp.bfloat16)
    loads[4].wait()
    bias[:, pl.ds(0, rows)] = jnp.where(patch < patch_count, 0.0, masked)
    page_turned[mine, :] = page_ref[:, mine].T
    part_recv[blk, grp] = jnp.zeros((piece, width), part_recv.dtype)
    query_rows[...] = jnp.zeros_like(query_rows)

    def forward(start, size):
        for hop in range(blocks - 1, 0, -1):
            remote(
                held.at[blk, pl.ds(start, size)], held.at[blk, pl.ds(start, size)], row_send,
                row_recv.at[blk], (partner(blk, hop, blocks), grp),
            )

    settle(held.at[blk, mate], column_recv.at[chip])
    forward(mate, 1)
    for step in range(1, chips):
        other = source(chip, step, chips)
        with jax.named_scope("w_col%d" % step):
            pl.when((chip != 1) | (other >= 1))(functools.partial(
                settle, held.at[blk, pl.ds(2 * other, 2)], column_recv.at[other]
            ))

        forward(2 * other, 2)

    settle(page_ref.at[:, theirs], mate_recv.at[0])
    settle(label_rows.at[1], mate_recv.at[1])
    bias[:, pl.ds(rows, rows)] = jnp.where(patch < label_rows[1, blocks], 0.0, masked)
    page_turned[theirs, :] = page_ref[:, theirs].T

    def both(value):
        return jnp.concatenate([value, value], axis=1)

    token_rows = both(token_row)

    def score_pass(query_pair):
        top = None
        for span in spans:
            scores = lax.dot_general(
                page_ref[span, :], query_pair, (((1,), (1,)), ((), ())),
                preferred_element_type=jnp.float32,
            )
            for start in range(0, span.size, patch_tile):
                part = scores[start:start + patch_tile]
                first = span.start + start
                if first >= free:
                    part = part + bias[pl.ds(first - free, patch_tile), :]
                part = fold(part)
                score_ref[0, pl.ds(first // 8, tile_folds)] = part
                part_top = jnp.max(part, axis=0)
                top = part_top if top is None else jnp.maximum(top, part_top)
        return top

    def exponent_pass(top):
        total = jnp.zeros((8, 2 * rows), jnp.float32)
        moment = jnp.zeros((8, 2 * rows), jnp.float32)
        span = patches // 8 // 2

        def body(index, carry):
            place = pl.ds(index * span, span)
            shifted = score_ref[0, place] - top
            exponent = jnp.exp2(shifted * exp2_scale)
            shifted_ref[0, place] = shifted
            exponent_ref[0, place] = exponent
            return (
                carry[0] + jnp.sum(exponent, axis=0), carry[1] + jnp.sum(exponent * shifted, axis=0)
            )

        return lax.fori_loop(0, 2, body, (total, moment))

    def pair_terms(top, total, moment, origin):
        row_max = jnp.max(top, axis=0, keepdims=True)
        gap = top - row_max
        scale = jnp.exp2(gap * exp2_scale)
        moment = scale * (moment + gap * total)
        total = jnp.sum(scale * total, axis=0, keepdims=True)
        shifted_score = jnp.sum(moment, axis=0, keepdims=True) / total
        token_score = shifted_score + row_max

        count_row = both(count_rows[origin])
        live = token_rows.astype(jnp.float32) < count_row
        live_score = jnp.where(live, token_score, 0.0)
        sublane = lax.broadcasted_iota(jnp.int32, (16, rows), 0)
        pieces = jnp.zeros((16, rows), jnp.float32)
        for page in range(2):
            remaining = live_score[:, page * rows:(page + 1) * rows]
            for index in range(3):
                value = remaining.astype(jnp.bfloat16).astype(jnp.float32)
                pieces = jnp.where(sublane == 8 * page + index, value, pieces)
                remaining = remaining - value
        piece_sums = jnp.dot(
            pieces.astype(jnp.bfloat16), same_query, preferred_element_type=jnp.float32
        )
        pair_sum = jnp.concatenate(
            [jnp.sum(piece_sums[8 * page:8 * page + 8], axis=0, keepdims=True) for page in range(2)],
            axis=1,
        )
        pair_score = pair_sum / count_row
        labels = jnp.concatenate([label_rows[0, origin], label_rows[1, origin]], axis=1)
        label_sign = 2.0 * labels - 1.0
        signed = -label_sign * (logit_scale * pair_score + logit_bias)
        decay = jnp.exp(-jnp.abs(signed))
        softplus = jnp.maximum(signed, 0.0) + jnp.log1p(decay)
        sigmoid = jnp.where(signed >= 0.0, 1.0, decay) / (1.0 + decay)
        loss_row = jnp.where(token_rows == 0, softplus, 0.0)
        token_grad = jnp.where(live, -label_sign * logit_scale * sigmoid / count_row, 0.0)
        slope = scale / total
        offset = slope * (1.0 + align_sharpness * (gap - shifted_score))
        return offset, slope * align_sharpness, token_grad, loss_row

    def block_terms(order, origin):
        queries = held[origin].reshape(rows, width)
        empty = jnp.zeros((rows, width), jnp.bfloat16)
        query_pair = jnp.concatenate([
            jnp.concatenate([queries, empty], axis=1), jnp.concatenate([empty, queries], axis=1)
        ], axis=0)
        columns = pl.ds(order * 2 * rows, 2 * rows)
        top = score_pass(query_pair)
        offset, slope, token_grad, loss_row = pair_terms(top, *exponent_pass(top), origin)
        token_grads[order] = token_grad
        for index, tile in enumerate(tiles):
            place = pl.ds(index * tile_folds, tile_folds)
            tile_grad = exponent_ref[slot, place] * (offset + slope * shifted_ref[slot, place])
            grads[tile, columns] = tile_grad.reshape(patch_tile, 2 * rows).astype(jnp.bfloat16)
        query_term = jnp.zeros((width, rows), jnp.float32)
        for span in spans:
            terms = jnp.dot(
                page_turned[:, span], grads[span, columns], preferred_element_type=jnp.float32
            )
            query_term = query_term + (
                terms[:width, :rows] * token_grad[:, :rows] + terms[width:, rows:] * token_grad[:, rows:]
            )
        return query_term.T, loss_row

    own, losses = block_terms(0, blk)
    own_term[...] = own.reshape(groups, piece, width)
    part_send[blk] = own.astype(jnp.bfloat16).reshape(groups, piece, width)
    for step in range(groups - 1, 0, -1):
        target = partner(grp, step, groups)
        remote(
            part_send.at[blk, target], part_recv.at[blk, grp], near_send, part_recv_sem.at[0],
            (blk, target),
        )

    for step in range(blocks - 1):
        origin = step + jnp.where(step >= blk, 1, 0)
        settle(held.at[origin], row_recv.at[origin])
        if step == 0:
            settle(count_rows.at[pl.ds(0, blocks - 1)], count_recv)
        query_term, block_losses = block_terms(step + 1, origin)
        losses = losses + block_losses
        part_send[origin] = query_term.astype(jnp.bfloat16).reshape(groups, piece, width)
        for target in range(groups):
            remote(
                part_send.at[origin, target], part_recv.at[blk, grp], far_send,
                part_recv_sem.at[1], (origin, target),
            )

    loss_send[...] = losses[:, rows:]
    remote(loss_send, loss_recv, loss_send_sem, loss_recv_sem, (blk, mate))
    same_row = (
        lax.broadcasted_iota(jnp.int32, (rows, rows), 0)
        == lax.broadcasted_iota(jnp.int32, (rows, rows), 1)
    )
    for order in range(blocks):
        origin = blk if order == 0 else order - 1 + jnp.where(order - 1 >= blk, 1, 0)
        queries = held[origin].reshape(rows, width)
        for page in range(2):
            spread_grad = jnp.where(same_row, token_grads[order, :, page * rows:(page + 1) * rows], 0.0)
            high = spread_grad.astype(jnp.bfloat16)
            low = (spread_grad - high.astype(jnp.float32)).astype(jnp.bfloat16)
            query_rows[
                pl.ds((order * 2 + page) * rows, rows), pl.ds(page * width, width)
            ] = jnp.dot(
                jnp.concatenate([high, low], axis=1), jnp.concatenate([queries, queries], axis=0),
                preferred_element_type=jnp.float32,
            ).astype(jnp.bfloat16)
    for span in spans:
        page_terms = jnp.dot(grads[span, :], query_rows[...], preferred_element_type=jnp.float32)
        page_send[span, :] = page_terms[:, width:].astype(jnp.bfloat16)
        page_grad_ref[span, :] = page_terms[:, :width]
        remote(
            page_send.at[span], page_recv.at[span], page_send_sem, page_recv_sem,
            (blk, mate),
        )
    settle(loss_recv, loss_recv_sem)
    loss_ref[0] = jnp.sum(losses[:, :rows] + loss_recv[...]) / jnp.float32(total_queries)
    settle(page_recv, page_recv_sem)
    page_grad_ref[...] = page_grad_ref[...] + page_recv[...].astype(jnp.float32)

    @pl.when(chip > 0)
    def _():
        settle(held.at[0, pl.ds(0, groups - 1)], column_send)

    @pl.when(chip == 0)
    def _():
        settle(held.at[0, pl.ds(0, 3)], column_send)

    @pl.when(chip == 1)
    def _():
        settle(held.at[0, pl.ds(0, 2 * (chips - 2))], relay_send)

    settle(held.at[pl.ds(0, blocks - 1)], row_send)
    settle(count_rows.at[pl.ds(0, blocks - 1)], count_send)
    settle(page_ref.at[:, theirs], mate_send.at[0])
    settle(extra_rows, mate_send.at[1])
    settle(part_send.at[0, pl.ds(0, groups - 1)], near_send)
    settle(part_send.at[pl.ds(0, blocks - 1)], far_send)
    settle(page_send, page_send_sem)
    settle(loss_send, loss_send_sem)

    sums = [jnp.zeros((piece, width), jnp.float32) for _ in range(2)]
    settle(part_recv.at[blk, pl.ds(0, groups - 1)], part_recv_sem.at[0])
    for group in range(groups):
        sums[group % 2] = sums[group % 2] + part_recv[blk, group].astype(jnp.float32)
    for step in range(blocks - 1):
        origin = step + jnp.where(step >= blk, 1, 0)
        if step == 0:
            settle(part_recv.at[pl.ds(0, blocks - 1)], part_recv_sem.at[1])
        for group in range(groups):
            sums[group % 2] = sums[group % 2] + part_recv[origin, group].astype(jnp.float32)
    for index in range(2):
        query_grad_ref[index] = sums[index]
    query_grad_ref[half] = query_grad_ref[half] + own_term[grp]


def write_out(query_grad_in, page_grad_in, loss_in, query_grad_ref, page_grad_ref, loss_ref, sems):
    copies = [
        pltpu.make_async_copy(page_grad_in, page_grad_ref, sems.at[0]),
        pltpu.make_async_copy(query_grad_in, query_grad_ref, sems.at[1]),
        pltpu.make_async_copy(loss_in, loss_ref, sems.at[2]),
    ]
    for copy in copies:
        copy.start()
    for copy in copies:
        copy.wait()


def local(queries, token_counts, pages, patch_counts, labels):
    blocks = lax.axis_size("blk")
    groups = lax.axis_size("grp")
    block_queries, slice_tokens, width = queries.shape
    patches = pages.shape[1]
    half_queries = block_queries // 2
    piece = half_queries * slice_tokens
    rows = piece * groups
    vmem = pl.BlockSpec(memory_space=pltpu.VMEM)
    smem = pl.BlockSpec(memory_space=pltpu.SMEM)
    anywhere = pl.BlockSpec(memory_space=pl.ANY)
    dma = pltpu.SemaphoreType.DMA
    f32, bf16 = jnp.float32, jnp.bfloat16
    query_grad, page_grad, page_loss = pl.pallas_call(
        functools.partial(kernel, blocks, groups, half_queries, slice_tokens),
        out_shape=(
            pltpu.VMEM((2, piece, width), f32),
            pltpu.VMEM((patches, width), f32),
            pltpu.SMEM((1,), f32),
        ),
        in_specs=[anywhere] * 5,
        out_specs=(vmem, vmem, smem),
        scratch_shapes=[
            pltpu.VMEM((2, piece, width), bf16),
            pltpu.SMEM(token_counts.shape, jnp.int32),
            pltpu.VMEM((patches, 2 * width), bf16),
            pltpu.VMEM((2 * width, patches), bf16),
            pltpu.SMEM((1,), jnp.int32),
            pltpu.SMEM((1, labels.shape[0]), jnp.int32),
            pltpu.VMEM((blocks, groups, piece, width), bf16),
            pltpu.VMEM((blocks * 2 * rows, 2 * width), bf16),
            pltpu.VMEM((blocks, 1, 2 * rows), f32),
            pltpu.VMEM((blocks, 1, rows), f32),
            pltpu.VMEM((2, blocks + 1, 1, rows), f32),
            pltpu.VMEM((blocks + 1, 1, rows), f32),
            pltpu.VMEM((patches - patches // 2, 2 * rows), f32),
            pltpu.VMEM((1, patches // 8, 8, 2 * rows), f32),
            pltpu.VMEM((1, patches // 8, 8, 2 * rows), f32),
            pltpu.VMEM((1, patches // 8, 8, 2 * rows), f32),
            pltpu.VMEM((patches, blocks * 2 * rows), bf16),
            pltpu.VMEM((groups, piece, width), f32),
            pltpu.VMEM((blocks, groups, piece, width), bf16),
            pltpu.VMEM((blocks, groups, piece, width), bf16),
            pltpu.VMEM((patches, width), bf16),
            pltpu.VMEM((patches, width), bf16),
            pltpu.VMEM((1, rows), f32),
            pltpu.VMEM((1, rows), f32),
            dma, dma((groups // 2,)), dma, dma((blocks,)), dma, dma,
            dma, pltpu.SemaphoreType.REGULAR, pltpu.SemaphoreType.REGULAR,
            dma((2,)), dma((2,)), dma, dma, dma((2,)),
            dma, dma, dma, dma, dma((5,)),
        ],
        compiler_params=pltpu.CompilerParams(
            collective_id=0, has_side_effects=True, vmem_limit_bytes=60 * 1024 * 1024
        ),
        name="late_interaction",
    )(queries.reshape(2, piece, width), token_counts, pages[0], patch_counts, labels.T)
    query_grad, page_grad, page_loss = pl.pallas_call(
        write_out,
        out_shape=(
            jax.ShapeDtypeStruct((2, piece, width), f32),
            jax.ShapeDtypeStruct((patches, width), f32),
            jax.ShapeDtypeStruct((1,), f32),
        ),
        in_specs=[anywhere] * 3,
        out_specs=(anywhere,) * 3,
        scratch_shapes=[dma((3,))],
        compiler_params=pltpu.CompilerParams(vmem_limit_bytes=1024 * 1024),
        name="write_out",
    )(query_grad, page_grad, page_loss)
    return query_grad.reshape(queries.shape), page_grad[None], page_loss


def solution(mesh):
    in_specs = (
        P("blk", "grp", None),
        P("blk"),
        P(("blk", "grp"), None, None),
        P(("blk", "grp")),
        P(None, ("blk", "grp")),
    )
    out_specs = (P("blk", "grp", None), P(("blk", "grp"), None, None), P(("blk", "grp")))
    return jax.shard_map(local, mesh=mesh, in_specs=in_specs, out_specs=out_specs, check_vma=False)
```

```python
import functools
import math

import jax
import jax.numpy as jnp
from jax import lax
from jax.experimental import pallas as pl
from jax.experimental.pallas import tpu as pltpu
from jax.sharding import PartitionSpec as P

align_sharpness = 4.0
logit_scale = 2.0
logit_bias = -5.0
masked = -1e30
exp2_scale = align_sharpness * math.log2(math.e)
MESH = pl.DeviceIdType.MESH
patch_tile = 256


def partner(position, step, size):
    if size & (size - 1):
        return lax.rem(position + step, size)
    result = 0
    bit = 1
    while bit < size:
        here = lax.rem(position // bit, 2)
        flip = (step // bit) % 2
        result = result + (1 - here if flip else here) * bit
        bit *= 2
    return result


def source(position, step, size):
    if size & (size - 1):
        return lax.rem(position + size - step, size)
    return partner(position, step, size)


def fold(value):
    return value.reshape(-1, 8, value.shape[1])


def kernel(
    blocks, groups, half_queries, slice_tokens,
    query_in, count_in, page_in, patch_count_in, label_in,
    query_grad_ref, page_grad_ref, loss_ref,
    query_ref, count_ref, page_ref, page_turned, patch_count_ref, label_ref,
    held, query_rows, token_grads, count_rows, label_rows, extra_rows, bias,
    score_ref, shifted_ref, exponent_ref, grads, own_term,
    part_send, part_recv, page_send, page_recv, loss_send, loss_recv,
    column_send, column_recv, row_send, row_recv, count_send, count_recv,
    relay_send, row_ready, column_ready, mate_send, mate_recv, near_send, far_send, part_recv_sem,
    page_send_sem, page_recv_sem, loss_send_sem, loss_recv_sem, load_sem,
):
    blk = lax.axis_index("blk")
    grp = lax.axis_index("grp")
    half = lax.rem(grp, 2)
    mate = grp + 1 - 2 * half
    patches, width = page_in.shape
    piece = half_queries * slice_tokens
    rows = piece * groups
    free = patches // 2
    total_queries = blocks * half_queries * 2
    tiles = [pl.ds(start, patch_tile) for start in range(0, patches, patch_tile)]
    tile_folds = patch_tile // 8
    slot = jnp.minimum(grp, 0)
    spans = [pl.ds(start, patches // 2) for start in (0, patches // 2)]
    mine, theirs = pl.ds(0, width), pl.ds(width, width)

    chip = grp // 2
    chips = groups // 2
    barrier = pltpu.get_barrier_semaphore()

    def greet(sem, device):
        pl.semaphore_signal(sem, inc=1, device_id=device, device_id_type=MESH)

    for step in range(1, groups):
        target = partner(grp, step, groups)
        pl.when(target // 2 >= chip - 1)(
            functools.partial(greet, barrier, (blk, target))
        )
    for step in range(1, blocks):
        target = partner(blk, step, blocks)
        pl.when(target > blk)(functools.partial(greet, barrier, (target, grp)))

    loads = [
        pltpu.make_async_copy(src, dst, load_sem.at[index])
        for index, (src, dst) in enumerate((
            (count_in, count_ref), (label_in, label_ref), (patch_count_in, patch_count_ref),
            (query_in, query_ref), (page_in, page_ref.at[:, mine]),
        ))
    ]
    for index in (3, 0, 1, 2, 4):
        loads[index].start()

    def remote(src, dst, send, recv, device):
        pltpu.make_async_remote_copy(
            src_ref=src, dst_ref=dst, send_sem=send, recv_sem=recv,
            device_id=device, device_id_type=MESH,
        ).start()

    def settle(ref, sem):
        pltpu.make_async_copy(ref, ref, sem).wait()

    def give_piece(target):
        remote(
            query_ref.at[lax.rem(target, 2)], held.at[blk, grp], column_send, column_recv.at[chip],
            (blk, target),
        )

    pl.semaphore_wait(barrier, 1 + 2 * chip + 2 * jnp.where(chip + 1 < chips, 1, 0) + blk)
    for step in range(1, blocks):
        target = partner(blk, step, blocks)
        pl.when(target < blk)(functools.partial(greet, row_ready, (target, grp)))
    for step in range(1, groups):
        target = partner(grp, step, groups)
        pl.when((target // 2 <= chip - 2) & (target >= 2))(
            functools.partial(greet, column_ready, (blk, target))
        )
    loads[3].wait()
    for step in range(1, groups):
        target = partner(grp, step, groups)
        pl.when(target // 2 <= chip + 1)(functools.partial(give_piece, target))
    held[blk, grp] = query_ref[half]
    remote(page_in, page_ref.at[:, theirs], mate_send.at[0], mate_recv.at[0], (blk, mate))

    @pl.when((chip > 0) & (chip + 2 < chips))
    def _():
        pl.semaphore_wait(column_ready, 2 * (chips - 2 - chip))
        for step in range(1, groups):
            target = partner(grp, step, groups)
            pl.when(target // 2 > chip + 1)(functools.partial(give_piece, target))

    @pl.when(chip == 1)
    def _():
        pair = held.at[blk, pl.ds(0, 2)]
        settle(pair, column_recv.at[0])
        for target in range(chips - 1, 1, -1):
            remote(pair, pair, relay_send, column_recv.at[0], (blk, 2 * target + half))

    @pl.when(blk + 1 < blocks)
    def _():
        pl.semaphore_wait(row_ready, blocks - 1 - blk)

    for step in range(blocks - 1, 0, -1):
        other = partner(blk, step, blocks)
        remote(query_ref.at[half], held.at[blk, grp], row_send, row_recv.at[blk], (other, grp))

    lane = lax.broadcasted_iota(jnp.int32, (1, rows), 1)
    query_row = lax.rem(lane // slice_tokens, half_queries)
    token_row = lane // piece * slice_tokens + lax.rem(lane, slice_tokens)

    def spread(read):
        result = jnp.zeros((1, rows), jnp.float32)
        for index in range(half_queries):
            result = jnp.where(query_row == index, read(index).astype(jnp.float32), result)
        return result

    for load in loads[:3]:
        load.wait()
    count_rows[blk] = spread(lambda index: count_ref[half * half_queries + index])
    for index in range(blocks):
        first = index * half_queries * 2
        label_rows[0, index] = spread(
            lambda query: label_ref[0, first + half * half_queries + query]
        )
        extra_rows[index] = spread(
            lambda query: label_ref[0, first + (1 - half) * half_queries + query]
        )
    patch_count = patch_count_ref[0].astype(jnp.float32)
    extra_rows[blocks] = jnp.full((1, rows), patch_count, jnp.float32)
    for step in range(blocks - 1, 0, -1):
        other = partner(blk, step, blocks)
        remote(count_rows.at[blk], count_rows.at[blk], count_send, count_recv, (other, grp))
    remote(extra_rows, label_rows.at[1], mate_send.at[1], mate_recv.at[1], (blk, mate))

    patch = (free + lax.broadcasted_iota(jnp.int32, (patches - free, rows), 0)).astype(jnp.float32)
    same_query = (
        lax.rem(lax.broadcasted_iota(jnp.int32, (rows, rows), 0) // slice_tokens, half_queries)
        == lax.rem(lax.broadcasted_iota(jnp.int32, (rows, rows), 1) // slice_tokens, half_queries)
    )
    same_query = jnp.where(same_query, 1.0, 0.0).astype(jnp.bfloat16)
    loads[4].wait()
    bias[:, pl.ds(0, rows)] = jnp.where(patch < patch_count, 0.0, masked)
    page_turned[mine, :] = page_ref[:, mine].T
    part_recv[blk, grp] = jnp.zeros((piece, width), part_recv.dtype)
    query_rows[...] = jnp.zeros_like(query_rows)

    def forward(start, size):
        for hop in range(blocks - 1, 0, -1):
            remote(
                held.at[blk, pl.ds(start, size)], held.at[blk, pl.ds(start, size)], row_send,
                row_recv.at[blk], (partner(blk, hop, blocks), grp),
            )

    settle(held.at[blk, mate], column_recv.at[chip])
    forward(mate, 1)
    for step in range(1, chips):
        other = source(chip, step, chips)
        with jax.named_scope("w_col%d" % step):
            pl.when((chip != 1) | (other >= 1))(functools.partial(
                settle, held.at[blk, pl.ds(2 * other, 2)], column_recv.at[other]
            ))

        forward(2 * other, 2)

    settle(page_ref.at[:, theirs], mate_recv.at[0])
    settle(label_rows.at[1], mate_recv.at[1])
    bias[:, pl.ds(rows, rows)] = jnp.where(patch < label_rows[1, blocks], 0.0, masked)
    page_turned[theirs, :] = page_ref[:, theirs].T

    def both(value):
        return jnp.concatenate([value, value], axis=1)

    token_rows = both(token_row)

    def score_pass(query_pair):
        top = None
        for span in spans:
            scores = lax.dot_general(
                page_ref[span, :], query_pair, (((1,), (1,)), ((), ())),
                preferred_element_type=jnp.float32,
            )
            for start in range(0, span.size, patch_tile):
                part = scores[start:start + patch_tile]
                first = span.start + start
                if first >= free:
                    part = part + bias[pl.ds(first - free, patch_tile), :]
                part = fold(part)
                score_ref[0, pl.ds(first // 8, tile_folds)] = part
                part_top = jnp.max(part, axis=0)
                top = part_top if top is None else jnp.maximum(top, part_top)
        return top

    def exponent_pass(top):
        total = jnp.zeros((8, 2 * rows), jnp.float32)
        moment = jnp.zeros((8, 2 * rows), jnp.float32)
        span = patches // 8 // 2

        def body(index, carry):
            place = pl.ds(index * span, span)
            shifted = score_ref[0, place] - top
            exponent = jnp.exp2(shifted * exp2_scale)
            shifted_ref[0, place] = shifted
            exponent_ref[0, place] = exponent
            return (
                carry[0] + jnp.sum(exponent, axis=0), carry[1] + jnp.sum(exponent * shifted, axis=0)
            )

        return lax.fori_loop(0, 2, body, (total, moment))

    def pair_terms(top, total, moment, origin):
        row_max = jnp.max(top, axis=0, keepdims=True)
        gap = top - row_max
        scale = jnp.exp2(gap * exp2_scale)
        moment = scale * (moment + gap * total)
        total = jnp.sum(scale * total, axis=0, keepdims=True)
        shifted_score = jnp.sum(moment, axis=0, keepdims=True) / total
        token_score = shifted_score + row_max

        count_row = both(count_rows[origin])
        live = token_rows.astype(jnp.float32) < count_row
        live_score = jnp.where(live, token_score, 0.0)
        sublane = lax.broadcasted_iota(jnp.int32, (16, rows), 0)
        pieces = jnp.zeros((16, rows), jnp.float32)
        for page in range(2):
            remaining = live_score[:, page * rows:(page + 1) * rows]
            for index in range(3):
                value = remaining.astype(jnp.bfloat16).astype(jnp.float32)
                pieces = jnp.where(sublane == 8 * page + index, value, pieces)
                remaining = remaining - value
        piece_sums = jnp.dot(
            pieces.astype(jnp.bfloat16), same_query, preferred_element_type=jnp.float32
        )
        pair_sum = jnp.concatenate(
            [jnp.sum(piece_sums[8 * page:8 * page + 8], axis=0, keepdims=True) for page in range(2)],
            axis=1,
        )
        pair_score = pair_sum / count_row
        labels = jnp.concatenate([label_rows[0, origin], label_rows[1, origin]], axis=1)
        label_sign = 2.0 * labels - 1.0
        signed = -label_sign * (logit_scale * pair_score + logit_bias)
        decay = jnp.exp(-jnp.abs(signed))
        softplus = jnp.maximum(signed, 0.0) + jnp.log1p(decay)
        sigmoid = jnp.where(signed >= 0.0, 1.0, decay) / (1.0 + decay)
        loss_row = jnp.where(token_rows == 0, softplus, 0.0)
        token_grad = jnp.where(live, -label_sign * logit_scale * sigmoid / count_row, 0.0)
        slope = scale / total
        offset = slope * (1.0 + align_sharpness * (gap - shifted_score))
        return offset, slope * align_sharpness, token_grad, loss_row

    def block_terms(order, origin):
        queries = held[origin].reshape(rows, width)
        empty = jnp.zeros((rows, width), jnp.bfloat16)
        query_pair = jnp.concatenate([
            jnp.concatenate([queries, empty], axis=1), jnp.concatenate([empty, queries], axis=1)
        ], axis=0)
        columns = pl.ds(order * 2 * rows, 2 * rows)
        top = score_pass(query_pair)
        offset, slope, token_grad, loss_row = pair_terms(top, *exponent_pass(top), origin)
        token_grads[order] = token_grad
        for index, tile in enumerate(tiles):
            place = pl.ds(index * tile_folds, tile_folds)
            tile_grad = exponent_ref[slot, place] * (offset + slope * shifted_ref[slot, place])
            grads[tile, columns] = tile_grad.reshape(patch_tile, 2 * rows).astype(jnp.bfloat16)
        query_term = jnp.zeros((width, rows), jnp.float32)
        for page, side in enumerate((mine, theirs)):
            terms = jnp.dot(
                page_turned[side, :], grads[:, columns], preferred_element_type=jnp.float32
            )
            lanes = slice(page * rows, (page + 1) * rows)
            query_term = query_term + terms[:, lanes] * token_grad[:, lanes]
        return query_term.T, loss_row

    own, losses = block_terms(0, blk)
    own_term[...] = own.reshape(groups, piece, width)
    part_send[blk] = own.astype(jnp.bfloat16).reshape(groups, piece, width)
    for step in range(groups - 1, 0, -1):
        target = partner(grp, step, groups)
        remote(
            part_send.at[blk, target], part_recv.at[blk, grp], near_send, part_recv_sem.at[0],
            (blk, target),
        )

    for step in range(blocks - 1):
        origin = step + jnp.where(step >= blk, 1, 0)
        settle(held.at[origin], row_recv.at[origin])
        if step == 0:
            settle(count_rows.at[pl.ds(0, blocks - 1)], count_recv)
        query_term, block_losses = block_terms(step + 1, origin)
        losses = losses + block_losses
        part_send[origin] = query_term.astype(jnp.bfloat16).reshape(groups, piece, width)
        for target in range(groups):
            remote(
                part_send.at[origin, target], part_recv.at[blk, grp], far_send,
                part_recv_sem.at[1], (origin, target),
            )

    loss_send[...] = losses[:, rows:]
    remote(loss_send, loss_recv, loss_send_sem, loss_recv_sem, (blk, mate))
    same_row = (
        lax.broadcasted_iota(jnp.int32, (rows, rows), 0)
        == lax.broadcasted_iota(jnp.int32, (rows, rows), 1)
    )
    for order in range(blocks):
        origin = blk if order == 0 else order - 1 + jnp.where(order - 1 >= blk, 1, 0)
        queries = held[origin].reshape(rows, width)
        for page in range(2):
            spread_grad = jnp.where(same_row, token_grads[order, :, page * rows:(page + 1) * rows], 0.0)
            high = spread_grad.astype(jnp.bfloat16)
            low = (spread_grad - high.astype(jnp.float32)).astype(jnp.bfloat16)
            query_rows[
                pl.ds((order * 2 + page) * rows, rows), pl.ds(page * width, width)
            ] = jnp.dot(
                jnp.concatenate([high, low], axis=1), jnp.concatenate([queries, queries], axis=0),
                preferred_element_type=jnp.float32,
            ).astype(jnp.bfloat16)
    for span in spans:
        page_terms = jnp.dot(grads[span, :], query_rows[...], preferred_element_type=jnp.float32)
        page_send[span, :] = page_terms[:, width:].astype(jnp.bfloat16)
        page_grad_ref[span, :] = page_terms[:, :width]
        remote(
            page_send.at[span], page_recv.at[span], page_send_sem, page_recv_sem,
            (blk, mate),
        )
    settle(loss_recv, loss_recv_sem)
    loss_ref[0] = jnp.sum(losses[:, :rows] + loss_recv[...]) / jnp.float32(total_queries)
    settle(page_recv, page_recv_sem)
    page_grad_ref[...] = page_grad_ref[...] + page_recv[...].astype(jnp.float32)

    @pl.when(chip > 0)
    def _():
        settle(held.at[0, pl.ds(0, groups - 1)], column_send)

    @pl.when(chip == 0)
    def _():
        settle(held.at[0, pl.ds(0, 3)], column_send)

    @pl.when(chip == 1)
    def _():
        settle(held.at[0, pl.ds(0, 2 * (chips - 2))], relay_send)

    settle(held.at[pl.ds(0, blocks - 1)], row_send)
    settle(count_rows.at[pl.ds(0, blocks - 1)], count_send)
    settle(page_ref.at[:, theirs], mate_send.at[0])
    settle(extra_rows, mate_send.at[1])
    settle(part_send.at[0, pl.ds(0, groups - 1)], near_send)
    settle(part_send.at[pl.ds(0, blocks - 1)], far_send)
    settle(page_send, page_send_sem)
    settle(loss_send, loss_send_sem)

    sums = [jnp.zeros((piece, width), jnp.float32) for _ in range(2)]
    settle(part_recv.at[blk, pl.ds(0, groups - 1)], part_recv_sem.at[0])
    for group in range(groups):
        sums[group % 2] = sums[group % 2] + part_recv[blk, group].astype(jnp.float32)
    for step in range(blocks - 1):
        origin = step + jnp.where(step >= blk, 1, 0)
        if step == 0:
            settle(part_recv.at[pl.ds(0, blocks - 1)], part_recv_sem.at[1])
        for group in range(groups):
            sums[group % 2] = sums[group % 2] + part_recv[origin, group].astype(jnp.float32)
    for index in range(2):
        query_grad_ref[index] = sums[index]
    query_grad_ref[half] = query_grad_ref[half] + own_term[grp]


def write_out(query_grad_in, page_grad_in, loss_in, query_grad_ref, page_grad_ref, loss_ref, sems):
    copies = [
        pltpu.make_async_copy(page_grad_in, page_grad_ref, sems.at[0]),
        pltpu.make_async_copy(query_grad_in, query_grad_ref, sems.at[1]),
        pltpu.make_async_copy(loss_in, loss_ref, sems.at[2]),
    ]
    for copy in copies:
        copy.start()
    for copy in copies:
        copy.wait()


def local(queries, token_counts, pages, patch_counts, labels):
    blocks = lax.axis_size("blk")
    groups = lax.axis_size("grp")
    block_queries, slice_tokens, width = queries.shape
    patches = pages.shape[1]
    half_queries = block_queries // 2
    piece = half_queries * slice_tokens
    rows = piece * groups
    vmem = pl.BlockSpec(memory_space=pltpu.VMEM)
    smem = pl.BlockSpec(memory_space=pltpu.SMEM)
    anywhere = pl.BlockSpec(memory_space=pl.ANY)
    dma = pltpu.SemaphoreType.DMA
    f32, bf16 = jnp.float32, jnp.bfloat16
    query_grad, page_grad, page_loss = pl.pallas_call(
        functools.partial(kernel, blocks, groups, half_queries, slice_tokens),
        out_shape=(
            pltpu.VMEM((2, piece, width), f32),
            pltpu.VMEM((patches, width), f32),
            pltpu.SMEM((1,), f32),
        ),
        in_specs=[anywhere] * 5,
        out_specs=(vmem, vmem, smem),
        scratch_shapes=[
            pltpu.VMEM((2, piece, width), bf16),
            pltpu.SMEM(token_counts.shape, jnp.int32),
            pltpu.VMEM((patches, 2 * width), bf16),
            pltpu.VMEM((2 * width, patches), bf16),
            pltpu.SMEM((1,), jnp.int32),
            pltpu.SMEM((1, labels.shape[0]), jnp.int32),
            pltpu.VMEM((blocks, groups, piece, width), bf16),
            pltpu.VMEM((blocks * 2 * rows, 2 * width), bf16),
            pltpu.VMEM((blocks, 1, 2 * rows), f32),
            pltpu.VMEM((blocks, 1, rows), f32),
            pltpu.VMEM((2, blocks + 1, 1, rows), f32),
            pltpu.VMEM((blocks + 1, 1, rows), f32),
            pltpu.VMEM((patches - patches // 2, 2 * rows), f32),
            pltpu.VMEM((1, patches // 8, 8, 2 * rows), f32),
            pltpu.VMEM((1, patches // 8, 8, 2 * rows), f32),
            pltpu.VMEM((1, patches // 8, 8, 2 * rows), f32),
            pltpu.VMEM((patches, blocks * 2 * rows), bf16),
            pltpu.VMEM((groups, piece, width), f32),
            pltpu.VMEM((blocks, groups, piece, width), bf16),
            pltpu.VMEM((blocks, groups, piece, width), bf16),
            pltpu.VMEM((patches, width), bf16),
            pltpu.VMEM((patches, width), bf16),
            pltpu.VMEM((1, rows), f32),
            pltpu.VMEM((1, rows), f32),
            dma, dma((groups // 2,)), dma, dma((blocks,)), dma, dma,
            dma, pltpu.SemaphoreType.REGULAR, pltpu.SemaphoreType.REGULAR,
            dma((2,)), dma((2,)), dma, dma, dma((2,)),
            dma, dma, dma, dma, dma((5,)),
        ],
        compiler_params=pltpu.CompilerParams(
            collective_id=0, has_side_effects=True, vmem_limit_bytes=60 * 1024 * 1024
        ),
        name="late_interaction",
    )(queries.reshape(2, piece, width), token_counts, pages[0], patch_counts, labels.T)
    query_grad, page_grad, page_loss = pl.pallas_call(
        write_out,
        out_shape=(
            jax.ShapeDtypeStruct((2, piece, width), f32),
            jax.ShapeDtypeStruct((patches, width), f32),
            jax.ShapeDtypeStruct((1,), f32),
        ),
        in_specs=[anywhere] * 3,
        out_specs=(anywhere,) * 3,
        scratch_shapes=[dma((3,))],
        compiler_params=pltpu.CompilerParams(vmem_limit_bytes=1024 * 1024),
        name="write_out",
    )(query_grad, page_grad, page_loss)
    return query_grad.reshape(queries.shape), page_grad[None], page_loss


def solution(mesh):
    in_specs = (
        P("blk", "grp", None),
        P("blk"),
        P(("blk", "grp"), None, None),
        P(("blk", "grp")),
        P(None, ("blk", "grp")),
    )
    out_specs = (P("blk", "grp", None), P(("blk", "grp"), None, None), P(("blk", "grp")))
    return jax.shard_map(local, mesh=mesh, in_specs=in_specs, out_specs=out_specs, check_vma=False)
```
